8 devices in a mesh: rep: 1 (over z), mp: 2 (over y), tok: 4 (over x, core).
Axes of the slice: x: 2, y: 2, z: 1, core: 2. Of those that a mesh axis runs over, the one named last changes fastest.
Arguments:
- x_in: bfloat16 [2, 512, 5120], P(None, ('rep', 'tok', 'mp'))
- seg_ids: int32 [2, 512], P(None, ('rep', 'tok', 'mp'))
- g_attn: bfloat16 [2, 5120], replicated
- w_q: bfloat16 [2, 5120, 40, 128], P(None, 'tok', 'mp')
- w_k: bfloat16 [2, 5120, 40, 128], P(None, 'tok', 'mp')
- w_v: bfloat16 [2, 5120, 40, 128], P(None, 'tok', 'mp')
- w_o: bfloat16 [2, 40, 128, 5120], P(None, 'mp', None, 'tok')
- g_mlp: bfloat16 [2, 5120], replicated
- w_gate: bfloat16 [2, 5120, 13824], P(None, 'tok', 'mp')
- w_up: bfloat16 [2, 5120, 13824], P(None, 'tok', 'mp')
- w_down: bfloat16 [2, 13824, 5120], P(None, 'mp', 'tok')
Outputs:
- output: float32 [2, 512, 5120], P(None, ('rep', 'tok', 'mp'))
All inputs are finite; a program needn't handle non-finite values.
Results may differ from the reference program's by a relative error of at most 0.0061746.
Values are sent between devices in bfloat16 or wider.
A program may use at most 1 GiB of HBM per device.

```python
import jax
import jax.numpy as jnp
from jax import lax

EMBED_DIM = 5120
FFN_DIM = 13824
Q_HEADS = 40
KV_HEADS = 40
HEAD_DIM = 128
LAYERS = 2
MICRO_BATCHES = 2
NUM_SHARDS = 4
BLOCK_LEN = 128
CUT_COUNT = 2
WAVE_COUNT = 4
TOKENS = NUM_SHARDS * BLOCK_LEN
BLOCKS = MICRO_BATCHES * NUM_SHARDS
NORM_EPS = 1e-5
ROPE_BASE = 10000.0
NEG_BIG = -1e30


def draw_segments(seg_key):
    cut_at = jax.random.randint(seg_key, (BLOCKS, CUT_COUNT), 1, BLOCK_LEN, dtype=jnp.int32)
    tok_order = jnp.arange(BLOCK_LEN, dtype=jnp.int32)
    is_start = jnp.any(tok_order[None, None, :] == cut_at[:, :, None], axis=1) | (tok_order[None, :] == 0)
    local_ids = jnp.cumsum(is_start.astype(jnp.int32), axis=1) - 1
    base_ids = jnp.arange(BLOCKS, dtype=jnp.int32)[:, None] * BLOCK_LEN
    return (local_ids + base_ids).astype(jnp.int32).reshape(MICRO_BATCHES, TOKENS)


def setup_inputs(seed: int = 0, part: int = 0) -> dict:
    root_key = jax.random.key(seed)
    key_list = jax.random.split(root_key, 12)
    part_key = jax.random.fold_in(key_list[0], part)
    noise_key, cos_key, sin_key, seg_key = jax.random.split(part_key, 4)
    freq_n = jnp.arange(1, WAVE_COUNT + 1, dtype=jnp.float32)
    t_frac = jnp.arange(BLOCK_LEN, dtype=jnp.float32) / BLOCK_LEN
    angles = 2.0 * jnp.pi * freq_n[:, None] * t_frac[None, :]
    amp_cos = jax.random.normal(cos_key, (BLOCKS, WAVE_COUNT, EMBED_DIM), jnp.float32)
    amp_sin = jax.random.normal(sin_key, (BLOCKS, WAVE_COUNT, EMBED_DIM), jnp.float32)
    smooth = (jnp.einsum('ks,bke->bse', jnp.cos(angles), amp_cos) + jnp.einsum('ks,bke->bse', jnp.sin(angles), amp_sin)) * WAVE_COUNT ** -0.5
    noise = jax.random.normal(noise_key, (BLOCKS, BLOCK_LEN, EMBED_DIM), jnp.float32)
    x_in = (0.8 * smooth + 0.6 * noise).reshape(MICRO_BATCHES, TOKENS, EMBED_DIM).astype(jnp.bfloat16)

    def weight(wkey, shape, fan_in):
        return (jax.random.normal(wkey, shape, jnp.float32) * fan_in ** -0.5).astype(jnp.bfloat16)

    def gains(wkey):
        return jax.random.uniform(wkey, (LAYERS, EMBED_DIM), jnp.float32, minval=0.5, maxval=1.5).astype(jnp.bfloat16)

    return {
        'x_in': x_in,
        'seg_ids': draw_segments(seg_key),
        'g_attn': gains(key_list[1]),
        'w_q': weight(key_list[2], (LAYERS, EMBED_DIM, Q_HEADS, HEAD_DIM), EMBED_DIM),
        'w_k': weight(key_list[3], (LAYERS, EMBED_DIM, KV_HEADS, HEAD_DIM), EMBED_DIM),
        'w_v': weight(key_list[4], (LAYERS, EMBED_DIM, KV_HEADS, HEAD_DIM), EMBED_DIM),
        'w_o': weight(key_list[5], (LAYERS, Q_HEADS, HEAD_DIM, EMBED_DIM), Q_HEADS * HEAD_DIM),
        'g_mlp': gains(key_list[6]),
        'w_gate': weight(key_list[7], (LAYERS, EMBED_DIM, FFN_DIM), EMBED_DIM),
        'w_up': weight(key_list[8], (LAYERS, EMBED_DIM, FFN_DIM), EMBED_DIM),
        'w_down': weight(key_list[9], (LAYERS, FFN_DIM, EMBED_DIM), FFN_DIM),
    }


def rms_norm(resid, gain_vec):
    mean_sq = jnp.mean(resid * resid, axis=-1, keepdims=True)
    return (resid * lax.rsqrt(mean_sq + NORM_EPS) * gain_vec.astype(jnp.float32)).astype(jnp.bfloat16)


def seg_positions(seg_rows):
    positions = jnp.arange(seg_rows.shape[-1], dtype=jnp.int32)
    previous = jnp.concatenate([seg_rows[..., :1] - 1, seg_rows[..., :-1]], axis=-1)
    start_at = jnp.where(seg_rows != previous, positions, 0)
    return positions - lax.cummax(start_at, axis=seg_rows.ndim - 1)


def rope_tables(positions, head_dim):
    half_dim = head_dim // 2
    inv_freq = ROPE_BASE ** (-2.0 * jnp.arange(half_dim, dtype=jnp.float32) / head_dim)
    angles = positions.astype(jnp.float32)[..., None] * inv_freq
    return jnp.cos(angles), jnp.sin(angles)


def apply_rope(values, cos_t, sin_t):
    half_dim = values.shape[-1] // 2
    first_half = values[..., :half_dim]
    second_half = values[..., half_dim:]
    return jnp.concatenate([first_half * cos_t - second_half * sin_t, second_half * cos_t + first_half * sin_t], axis=-1)


def block_attention(operands):
    q_blk, k_blk, v_blk, seg_blk = operands
    tok_order = jnp.arange(BLOCK_LEN)
    allowed = (seg_blk[:, None] == seg_blk[None, :]) & (tok_order[None, :] <= tok_order[:, None])

    def one_group(group_ops):
        q_grp, k_grp, v_grp = group_ops
        scores = jnp.einsum('sgd,td->sgt', q_grp.astype(jnp.float32), k_grp.astype(jnp.float32)) * HEAD_DIM ** -0.5
        scores = jnp.where(allowed[:, None, :], scores, NEG_BIG)
        probs_bf = jax.nn.softmax(scores, axis=-1).astype(jnp.bfloat16)
        return jnp.einsum('sgt,td->sgd', probs_bf.astype(jnp.float32), v_grp.astype(jnp.float32)).astype(jnp.bfloat16)

    group_out = lax.map(one_group, (jnp.moveaxis(q_blk, 1, 0), jnp.moveaxis(k_blk, 1, 0), jnp.moveaxis(v_blk, 1, 0)))
    return jnp.moveaxis(group_out, 0, 1)


def reference(x_in, seg_ids, g_attn, w_q, w_k, w_v, w_o, g_mlp, w_gate, w_up, w_down):
    groups = Q_HEADS // KV_HEADS
    seg_blocks = seg_ids.reshape(BLOCKS, BLOCK_LEN)
    cos_t, sin_t = rope_tables(seg_positions(seg_blocks), HEAD_DIM)
    cos_t = cos_t[:, :, None, :]
    sin_t = sin_t[:, :, None, :]

    def layer_step(residual, layer_w):
        ga_vec, wq_l, wk_l, wv_l, wo_l, gm_vec, wg_l, wu_l, wd_l = layer_w
        hidden = rms_norm(residual, ga_vec).reshape(BLOCKS, BLOCK_LEN, EMBED_DIM).astype(jnp.float32)
        q_lin = jnp.einsum('bse,end->bsnd', hidden, wq_l.astype(jnp.float32))
        k_lin = jnp.einsum('bse,end->bsnd', hidden, wk_l.astype(jnp.float32))
        v_lin = jnp.einsum('bse,end->bsnd', hidden, wv_l.astype(jnp.float32))
        q_rot = apply_rope(q_lin, cos_t, sin_t).astype(jnp.bfloat16).reshape(BLOCKS, BLOCK_LEN, KV_HEADS, groups, HEAD_DIM)
        k_rot = apply_rope(k_lin, cos_t, sin_t).astype(jnp.bfloat16)
        v_val = v_lin.astype(jnp.bfloat16)
        attn_out = lax.map(block_attention, (q_rot, k_rot, v_val, seg_blocks))
        attn_out = attn_out.reshape(BLOCKS, BLOCK_LEN, Q_HEADS, HEAD_DIM).astype(jnp.float32)
        proj_out = jnp.einsum('bsnd,nde->bse', attn_out, wo_l.astype(jnp.float32))
        residual = residual + proj_out.reshape(MICRO_BATCHES, TOKENS, EMBED_DIM)
        hidden = rms_norm(residual, gm_vec).reshape(MICRO_BATCHES * TOKENS, EMBED_DIM)
        gate_val = jnp.dot(hidden, wg_l, preferred_element_type=jnp.float32)
        up_val = jnp.dot(hidden, wu_l, preferred_element_type=jnp.float32)
        act_val = (jax.nn.silu(gate_val) * up_val).astype(jnp.bfloat16)
        down_val = jnp.dot(act_val, wd_l, preferred_element_type=jnp.float32)
        return residual + down_val.reshape(MICRO_BATCHES, TOKENS, EMBED_DIM), None

    final_res, _ = lax.scan(layer_step, x_in.astype(jnp.float32), (g_attn, w_q, w_k, w_v, w_o, g_mlp, w_gate, w_up, w_down))
    return final_res
```

```python
import jax
import jax.numpy as jnp
from jax import lax
from jax.sharding import PartitionSpec as P

NORM_EPS = 1e-5
ROPE_BASE = 10000.0
NEG_BIG = -1e30
F32 = jnp.float32
BF16 = jnp.bfloat16


def seg_positions(seg_rows):
    positions = jnp.arange(seg_rows.shape[-1], dtype=jnp.int32)
    previous = jnp.concatenate([seg_rows[..., :1] - 1, seg_rows[..., :-1]], axis=-1)
    start_at = jnp.where(seg_rows != previous, positions, 0)
    return positions - lax.cummax(start_at, axis=seg_rows.ndim - 1)


def rope_tables(positions, head_dim):
    half_dim = head_dim // 2
    inv_freq = ROPE_BASE ** (-2.0 * jnp.arange(half_dim, dtype=F32) / head_dim)
    angles = positions.astype(F32)[..., None] * inv_freq
    return jnp.cos(angles), jnp.sin(angles)


def apply_rope(values, cos_t, sin_t):
    half_dim = values.shape[-1] // 2
    a = values[..., :half_dim]
    b = values[..., half_dim:]
    return jnp.concatenate([a * cos_t - b * sin_t, b * cos_t + a * sin_t], axis=-1)


def dot(a, b):
    return lax.dot_general(a, b, (((a.ndim - 1,), (0,)), ((), ())), preferred_element_type=F32)


GU_CHUNKS = 3


def solution(mesh):
    act_spec = P(None, ('rep', 'tok', 'mp'), None)
    seg_spec = P(None, ('rep', 'tok', 'mp'))
    gain_spec = P(None, None)
    head_in = P(None, 'tok', 'mp', None)
    head_out = P(None, 'mp', None, 'tok')
    ffn_in = P(None, 'tok', 'mp')
    ffn_out = P(None, 'mp', 'tok')

    def to_x(v):
        return lax.ppermute(v, 'tok', [(i, i ^ 2) for i in range(4)])

    def to_c(v):
        return lax.ppermute(v, 'tok', [(i, i ^ 1) for i in range(4)])

    def to_xc(v):
        return lax.ppermute(v, 'tok', [(i, i ^ 3) for i in range(4)])

    def to_y(v):
        return lax.ppermute(v, 'mp', [(0, 1), (1, 0)])

    def device_fn(x_in, seg_ids, g_attn, w_q, w_k, w_v, w_o, g_mlp, w_gate, w_up, w_down):
        n_layers = w_q.shape[0]
        micro_n, loc_len, embed = x_in.shape
        feat = w_q.shape[1]
        heads, head_dim = w_q.shape[2], w_q.shape[3]
        h_half = heads // 2
        ffn = w_gate.shape[2]
        f_half = ffn // 2
        f_chunk = f_half // GU_CHUNKS
        t = lax.axis_index('tok')
        m = lax.axis_index('mp')
        core = t % 2
        xpos = t // 2

        seg_all = lax.all_gather(seg_ids, ('tok', 'mp'), axis=1, tiled=True)
        blk_len = 2 * loc_len
        seg_own = lax.dynamic_slice_in_dim(seg_all, xpos * 2 * blk_len, 2 * blk_len, 1).reshape(micro_n, 2, blk_len)
        pos_own = seg_positions(seg_own)
        in_blk = jnp.broadcast_to(jnp.arange(blk_len, dtype=jnp.int32), seg_own.shape)
        def half_first(v):
            v4 = v.reshape(micro_n, 2, 2, loc_len)
            return jnp.where(m == 0, v4, v4[:, :, ::-1]).reshape(micro_n, 2, blk_len)
        seg_own, pos_own, in_blk = half_first(seg_own), half_first(pos_own), half_first(in_blk)
        allowed = (seg_own[..., :, None] == seg_own[..., None, :]) & (in_blk[..., None, :] <= in_blk[..., :, None])
        cos_t, sin_t = rope_tables(pos_own, head_dim)

        def to_rows(v):
            d = v.shape[-1]
            return v.reshape(micro_n, 2, 2, loc_len, d).transpose(0, 2, 1, 3, 4).reshape(micro_n, 2 * blk_len, 1, d)
        cos_t, sin_t = to_rows(cos_t), to_rows(sin_t)

        def start_piece(mb, k):
            s = lax.dynamic_slice_in_dim(x_in[mb], (t ^ k) * feat, feat, 1)
            return s
        resid = []
        for mb in range(micro_n):
            p = [start_piece(mb, 0), to_c(start_piece(mb, 1)), to_x(start_piece(mb, 2)), to_xc(start_piece(mb, 3))]
            own = jnp.where(core == 0, jnp.stack([p[0], p[1]]), jnp.stack([p[1], p[0]]))
            oth = jnp.where(core == 0, jnp.stack([p[2], p[3]]), jnp.stack([p[3], p[2]]))
            resid.append(jnp.stack([own, oth]).astype(F32))

        def normed(r, gain):
            sq = jnp.sum(r * r, axis=-1)
            sq = sq + to_c(sq)
            sq = sq + to_x(sq)[::-1]
            scale = lax.rsqrt(sq / embed + NORM_EPS)
            g = lax.dynamic_slice_in_dim(gain, t * feat, feat, 0).astype(F32)
            h_loc = (r * scale[..., None] * g).astype(BF16)
            h_y = to_y(h_loc)
            h = jnp.stack([h_loc, h_y], axis=1).reshape(2, 2 * blk_len, feat)
            h_c = to_c(h)
            return h, h_c

        def swap_halves(w, half):
            own = lax.dynamic_slice_in_dim(w, core * half, half, 1)
            snd = lax.dynamic_slice_in_dim(w, (1 - core) * half, half, 1)
            return own, to_c(snd)

        def col_matmul(h, h_c, w_own, w_rcv):
            snd = dot(h[1], w_own) + dot(h_c[1], w_rcv)
            got = to_x(snd)
            return dot(h[0], w_own) + dot(h_c[0], w_rcv) + got

        def row_reduce(parts):
            half = blk_len
            snd = keep = None
            for a_own, a_oth, w in parts:
                mine = jnp.concatenate([a_own[:half], a_oth[:half]], axis=0)
                theirs = jnp.concatenate([a_own[half:], a_oth[half:]], axis=0)
                d_snd, d_keep = dot(theirs, w), dot(mine, w)
                snd = d_snd if snd is None else snd + d_snd
                keep = d_keep if keep is None else keep + d_keep
            return (keep + to_y(snd)).reshape(2, 2, loc_len, feat)

        for l in range(n_layers):
            qkv_w = []
            for w in (w_k, w_v, w_q):
                own, rcv = swap_halves(w[l], h_half)
                qkv_w.append((own.reshape(feat, -1), rcv.reshape(feat, -1)))
            gu_w = [swap_halves(w[l], f_half) for w in (w_gate, w_up)]
            wo = w_o[l].reshape(heads * head_dim, feat)
            hd = h_half * head_dim
            wo_own = lax.dynamic_slice_in_dim(wo, core * hd, hd, 0)
            wo_oth = lax.dynamic_slice_in_dim(wo, (1 - core) * hd, hd, 0)

            for mb in range(micro_n):
                h, h_c = normed(resid[mb], g_attn[l])
                k_lin, v_lin, q_lin = [col_matmul(h, h_c, *w).reshape(2 * blk_len, h_half, head_dim) for w in qkv_w]
                k_rot = apply_rope(k_lin, cos_t[mb], sin_t[mb]).astype(BF16)
                q_rot = apply_rope(q_lin, cos_t[mb], sin_t[mb]).astype(BF16)
                v_val = v_lin.astype(BF16)

                def blocks(v):
                    return v.reshape(2, 2, loc_len, h_half, head_dim).transpose(1, 0, 2, 3, 4).reshape(2, blk_len, h_half, head_dim)
                qb, kb, vb = blocks(q_rot), blocks(k_rot), blocks(v_val)
                scores = jnp.einsum('bsnd,btnd->bnst', qb, kb, preferred_element_type=F32) * head_dim ** -0.5
                scores = jnp.where(allowed[mb][:, None], scores, NEG_BIG)
                probs = jax.nn.softmax(scores, axis=-1).astype(BF16)
                o = jnp.einsum('bnst,btnd->bsnd', probs, vb, preferred_element_type=F32).astype(BF16)
                o = o.reshape(2, 2, loc_len, hd).transpose(1, 0, 2, 3).reshape(2 * blk_len, hd)
                o_x = to_x(o)
                o_c = to_c(o)
                o_xc = to_c(o_x)
                resid[mb] = resid[mb] + row_reduce([(o, o_x, wo_own), (o_c, o_xc, wo_oth)])

            for mb in range(micro_n):
                h, h_c = normed(resid[mb], g_mlp[l])
                parts = []
                for j in range(GU_CHUNKS):
                    sl = slice(j * f_chunk, (j + 1) * f_chunk)
                    gate, up = [col_matmul(h, h_c, w_own[:, sl], w_rcv[:, sl]) for w_own, w_rcv in gu_w]
                    act = (jax.nn.silu(gate) * up).astype(BF16)
                    a_x = to_x(act)
                    a_c = to_c(act)
                    a_xc = to_c(a_x)
                    wd_own = lax.dynamic_slice_in_dim(w_down[l], core * f_half + j * f_chunk, f_chunk, 0)
                    wd_oth = lax.dynamic_slice_in_dim(w_down[l], (1 - core) * f_half + j * f_chunk, f_chunk, 0)
                    parts += [(act, a_x, wd_own), (a_c, a_xc, wd_oth)]
                resid[mb] = resid[mb] + row_reduce(parts)

        outs = []
        for mb in range(micro_n):
            r = resid[mb]
            r = jnp.where(core == 0, r, r[:, ::-1])
            p = [r[0, 0], to_c(r[0, 1]), to_x(r[1, 0]), to_xc(r[1, 1])]
            row = jnp.zeros((loc_len, embed), F32)
            for k in range(4):
                row = lax.dynamic_update_slice_in_dim(row, p[k], (t ^ k) * feat, 1)
            outs.append(row)
        return jnp.stack(outs)

    return jax.shard_map(
        device_fn,
        mesh=mesh,
        in_specs=(act_spec, seg_spec, gain_spec, head_in, head_in, head_in, head_out, gain_spec, ffn_in, ffn_in, ffn_out),
        out_specs=act_spec,
        check_vma=False,
    )
```

```python
import functools

import jax
import jax.numpy as jnp
from jax import lax
from jax.experimental import pallas as pl
from jax.experimental.pallas import tpu as pltpu
from jax.sharding import PartitionSpec as P

NORM_EPS = 1e-5
ROPE_BASE = 10000.0
NEG_BIG = -1e30
F32 = jnp.float32
BF16 = jnp.bfloat16
MESH = pl.DeviceIdType.MESH


def seg_positions(seg_rows):
    positions = jnp.arange(seg_rows.shape[-1], dtype=jnp.int32)
    previous = jnp.concatenate([seg_rows[..., :1] - 1, seg_rows[..., :-1]], axis=-1)
    start_at = jnp.where(seg_rows != previous, positions, 0)
    return positions - lax.cummax(start_at, axis=seg_rows.ndim - 1)


def rope_tables(positions, head_dim):
    half_dim = head_dim // 2
    inv_freq = ROPE_BASE ** (-2.0 * jnp.arange(half_dim, dtype=F32) / head_dim)
    angles = positions.astype(F32)[..., None] * inv_freq
    return jnp.cos(angles), jnp.sin(angles)


def mm(a, b):
    return jnp.dot(a, b, preferred_element_type=F32)


FEAT = 1280
EMBED = 5120
HALF = 1280
FHALF = 3456
ROWS = 256
QB = 256
GB = 384
SW = 768
N_Q = HALF // QB
N_G = FHALF // GB
D_CHUNK = 3 * GB
N_D = FHALF // D_CHUNK
CB = 256


def body(n_layers, x_ref, cos_ref, sin_ref, mask_ref, gain_ref, wq, wk, wv, wo, wg, wu, wd,
         out_ref, qkvr, gur,
         R, H, HC, XS, XO, XR, W, WR, ACT, PB, YR, SQ, SQC, SQS, SQX,
         xs_s, xr_s, as_s, ar_s, acs_s, acr_s, ys_s, yr_s, hys_s, hyr_s, hcs_s, hcr_s,
         sqcs_s, sqcr_s, sqxs_s, sqxr_s, sws_s, swr_s, os_s, or_s, w_s, wr_s):
    m = lax.axis_index('mp')
    t = lax.axis_index('tok')
    core = lax.rem(t, 2)
    xpos = lax.div(t, 2)
    t_c = xpos * 2 + (1 - core)
    t_x = (1 - xpos) * 2 + core
    t_d = (1 - xpos) * 2 + (1 - core)
    rep = lax.axis_index('rep')
    dev = {'c': (rep, m, t_c), 'x': (rep, m, t_x), 'd': (rep, m, t_d), 'y': (rep, 1 - m, t)}

    barrier = pltpu.get_barrier_semaphore()
    for k in ('c', 'x', 'd', 'y'):
        pl.semaphore_signal(barrier, inc=1, device_id=dev[k], device_id_type=MESH)
    pl.semaphore_wait(barrier, 4)

    def rcopy(src, dst, ss, rs, to):
        return pltpu.make_async_remote_copy(src_ref=src, dst_ref=dst, send_sem=ss, recv_sem=rs,
                                            device_id=dev[to], device_id_type=MESH)

    def al(v, n=128):
        return pl.multiple_of(v, n)

    swaps = {}
    n_sw = [0]

    def swap_start(key, src, dst):
        i = n_sw[0]
        n_sw[0] += 1
        c = rcopy(src, dst, sws_s.at[i], swr_s.at[i], 'c')
        c.start()
        swaps[key] = [c, False]

    def swap_need(key):
        e = swaps[key]
        if not e[1]:
            e[0].wait()
            e[1] = True

    def swap_qkv(l, fine):
        for b in range(N_Q):
            for i, w in enumerate((wq, wk, wv)):
                if fine:
                    swap_start((l, 'qkv', i, b), w.at[l, :, pl.ds(al((1 - core) * HALF + b * QB), QB)],
                               qkvr.at[l, i, :, pl.ds(b * QB, QB)])
                elif b == 0:
                    swap_start((l, 'qkv', i), w.at[l, :, pl.ds(al((1 - core) * HALF), HALF)], qkvr.at[l, i])
        if not fine:
            for b in range(N_Q):
                for i in range(3):
                    swaps[(l, 'qkv', i, b)] = swaps[(l, 'qkv', i)]

    def swap_gu(l):
        for i, w in enumerate((wg, wu)):
            swap_start((l, 'gu', i), w.at[l, :, pl.ds(al((1 - core) * FHALF), FHALF)], gur.at[l, i])

    steps = []
    for l in range(n_layers):
        for mb in range(2):
            steps += [(l, mb, 'q', b) for b in range(N_Q)]
        for mb in range(2):
            steps += [(l, mb, 'g', b) for b in range(N_G)]

    def w_copies(k):
        l, mb, kind, b = steps[k]
        s = k % 2
        cs = []
        if kind == 'q':
            for i, w in enumerate((wq, wk, wv)):
                cs.append((w.at[l, :, pl.ds(al(core * HALF + b * QB), QB)], W.at[s, 0, :, pl.ds(i * QB, QB)]))
                cs.append((qkvr.at[l, i, :, pl.ds(b * QB, QB)], W.at[s, 1, :, pl.ds(i * QB, QB)]))
        else:
            for i, w in enumerate((wg, wu)):
                cs.append((w.at[l, :, pl.ds(al(core * FHALF + b * GB), GB)], W.at[s, 0, :, pl.ds(i * GB, GB)]))
                cs.append((gur.at[l, i, :, pl.ds(b * GB, GB)], W.at[s, 1, :, pl.ds(i * GB, GB)]))
        return [pltpu.make_async_copy(a, d, w_s.at[s, j]) for j, (a, d) in enumerate(cs)]

    w_live = {}

    def w_start(k):
        if k >= len(steps):
            return
        l, mb, kind, b = steps[k]
        if kind == 'q':
            for i in range(3):
                swap_need((l, 'qkv', i, b))
        else:
            for i in range(2):
                swap_need((l, 'gu', i))
        w_live[k] = w_copies(k)
        for c in w_live[k]:
            c.start()

    x_live = {}

    def issue(k):
        l, mb, kind, b = steps[k]
        s = k % 2
        for c in w_live.pop(k):
            c.wait()
        if k >= 2:
            x_live[k - 2].wait_send()

        def half(row0, dst):
            @pl.loop(0, SW // CB)
            def _(j):
                cols = pl.ds(al(j * CB, CB), CB)
                dst[s, :, cols] = (mm(H[mb, pl.ds(row0, ROWS), :], W[s, 0, :, cols])
                                   + mm(HC[mb, pl.ds(row0, ROWS), :], W[s, 1, :, cols]))
        half(ROWS, XS)
        x_live[k] = rcopy(XS.at[s], XR.at[k % 4], xs_s.at[s], xr_s.at[k % 4], 'x')
        x_live[k].start()
        half(0, XO)
        w_start(k + 2)

    a_live = {}

    def consume(k):
        l, mb, kind, b = steps[k]
        s, q = k % 2, k % 4
        x_live[k].wait_recv()
        if kind == 'q':
            cos, sin = cos_ref[mb], sin_ref[mb]
            for hh in range(QB // 128):
                def part(i):
                    c0 = i * QB + hh * 128
                    return XO[s, :, c0:c0 + 128] + XR[q, :, c0:c0 + 128]

                def rope(v):
                    return (v * cos + pltpu.roll(v, 64, 1) * sin).astype(BF16)
                qh, kh, vh = rope(part(0)), rope(part(1)), part(2).astype(BF16)
                sc = lax.dot_general(qh, kh, (((1,), (1,)), ((), ())), preferred_element_type=F32) * (128 ** -0.5)
                sc = jnp.where(mask_ref[mb] > 0.0, sc, NEG_BIG)
                e = jnp.exp(sc - jnp.max(sc, axis=-1, keepdims=True))
                p = (e / jnp.sum(e, axis=-1, keepdims=True)).astype(BF16)
                ACT[mb, 0, :, b * QB + hh * 128:b * QB + hh * 128 + 128] = mm(p, vh).astype(BF16)
            cols = pl.ds(b * QB, QB)
        else:
            g = XO[s, :, :GB] + XR[q, :, :GB]
            u = XO[s, :, GB:] + XR[q, :, GB:]
            ACT[mb, 0, :, b * GB:(b + 1) * GB] = (jax.nn.silu(g) * u).astype(BF16)
            cols = pl.ds(b * GB, GB)
        c = rcopy(ACT.at[mb, 0, :, cols], ACT.at[mb, 1, :, cols], as_s.at[mb, b], ar_s.at[mb, b], 'x')
        c.start()
        a_live[mb, b] = c

    row_seq = []
    for l in range(n_layers):
        row_seq += [(l, mb, 'o', 0) for mb in range(2)] + [(l, mb, 'd', j) for mb in range(2) for j in range(N_D)]
    row_live = {}

    def row_start(i):
        if i >= len(row_seq):
            return
        l, mb, kind, j = row_seq[i]
        if kind == 'o':
            n, src = HALF, lambda c: wo.at[l, pl.ds(al(c * HALF), HALF), :]
        else:
            n, src = D_CHUNK, lambda c: wd.at[l, pl.ds(al(c * FHALF + j * D_CHUNK), D_CHUNK), :]
        row_live[i] = [pltpu.make_async_copy(src(core), WR.at[0, pl.ds(0, n), :], wr_s.at[0]),
                       pltpu.make_async_copy(src(1 - core), WR.at[1, pl.ds(0, n), :], wr_s.at[1])]
        for c in row_live[i]:
            c.start()

    row_at = [0]

    def row_wait():
        for c in row_live.pop(row_at[0]):
            c.wait()

    def row_done():
        row_at[0] += 1
        row_start(row_at[0])

    def row_mm(mb, xs, a0, n, first):
        @pl.loop(0, FEAT // CB)
        def _(j):
            cols = pl.ds(al(j * CB, CB), CB)
            v = (mm(ACT[mb, xs, :, a0:a0 + n], WR[0, :n, cols])
                 + mm(ACT[mb, 2 + xs, :, a0:a0 + n], WR[1, :n, cols]))
            if first:
                PB[mb, xs, :, cols] = v
            else:
                PB[mb, xs, :, cols] += v

    ac_live = {}

    def act_to_core(mb, xs, j, a0, n):
        cols = pl.ds(a0, n)
        c = rcopy(ACT.at[mb, xs, :, cols], ACT.at[mb, 2 + xs, :, cols], acs_s.at[mb, j, xs], acr_s.at[mb, j, xs], 'c')
        c.start()
        ac_live[mb, j, xs] = c

    y_live = {}

    def y_send(mb, xs):
        c = rcopy(PB.at[mb, xs, pl.ds(128, 128), :], YR.at[mb, xs], ys_s.at[mb, xs], yr_s.at[mb, xs], 'y')
        c.start()
        y_live[mb, xs] = c

    def r_update(mb):
        for xs in range(2):
            y_live[mb, xs].wait()
            rows = slice(xs * 128, xs * 128 + 128)
            R[mb, rows, :] = R[mb, rows, :] + (PB[mb, xs, :128, :] + YR[mb, xs])

    n_live = {}

    def norm_squares(mb):
        acc = None
        for j in range(FEAT // 128):
            v = R[mb, :, j * 128:(j + 1) * 128]
            acc = v * v if acc is None else acc + v * v
        SQ[mb] = acc
        c = rcopy(SQ.at[mb], SQC.at[mb], sqcs_s.at[mb], sqcr_s.at[mb], 'c')
        c.start()
        c.wait()
        SQS[mb] = SQ[mb] + SQC[mb]
        c = rcopy(SQS.at[mb], SQX.at[mb], sqxs_s.at[mb], sqxr_s.at[mb], 'x')
        c.start()
        n_live[mb, 'sq'] = c

    def norm_apply(mb, gi):
        n_live[mb, 'sq'].wait()
        for xs in range(2):
            o = 1 - xs
            tot = SQS[mb, xs * 128:(xs + 1) * 128, :] + SQX[mb, o * 128:(o + 1) * 128, :]
            scale = lax.rsqrt(jnp.sum(tot, axis=-1, keepdims=True) / EMBED + NORM_EPS)
            h = R[mb, xs * 128:(xs + 1) * 128, :] * scale * gain_ref[gi:gi + 1, :]
            H[mb, xs * 256:xs * 256 + 128, :] = h.astype(BF16)
        for xs in range(2):
            mine, theirs = pl.ds(xs * 256, 128), pl.ds(xs * 256 + 128, 128)
            c = rcopy(H.at[mb, mine, :], H.at[mb, theirs, :], hys_s.at[mb, xs], hyr_s.at[mb, xs], 'y')
            c.start()
            n_live[mb, 'y', xs] = c
        for xs in range(2):
            mine = pl.ds(xs * 256, 128)
            c = rcopy(H.at[mb, mine, :], HC.at[mb, mine, :], hcs_s.at[mb, xs], hcr_s.at[mb, xs], 'c')
            c.start()
            n_live[mb, 'c', xs] = c

    def norm_finish(mb):
        for xs in range(2):
            n_live[mb, 'y', xs].wait()
            theirs = pl.ds(xs * 256 + 128, 128)
            c = rcopy(H.at[mb, theirs, :], HC.at[mb, theirs, :], hcs_s.at[mb, 2 + xs], hcr_s.at[mb, 2 + xs], 'c')
            c.start()
            n_live[mb, 'c', 2 + xs] = c
        for i in range(4):
            n_live[mb, 'c', i].wait()

    o_live = []

    def out_send(mb):
        cols = pl.ds(al(t * FEAT), FEAT)
        for i, (xs, flip, to) in enumerate(((1, 0, 'x'), (1, 1, 'd'), (0, 1, 'c'))):
            cp = core + flip * (1 - 2 * core)
            c = rcopy(R.at[mb, pl.ds(al(xs * 128 + cp * 64, 64), 64), :], out_ref.at[mb, :, cols],
                      os_s.at[mb, i], or_s.at[mb, i], to)
            c.start()
            o_live.append(c)
        c = pltpu.make_async_copy(R.at[mb, pl.ds(al(core * 64, 64), 64), :], out_ref.at[mb, :, cols], os_s.at[mb, 3])
        c.start()
        o_live.append(c)

    todo = {}

    def at(k, f, *args):
        todo.setdefault(k, []).append(functools.partial(f, *args))

    def tail_a(l, mb, kind):
        if kind == 'q':
            j, a0, n, first = 0, 0, HALF, True
        else:
            j, a0, n, first = N_D - 1, (N_D - 1) * D_CHUNK, D_CHUNK, False
        act_to_core(mb, 0, j, a0, n)
        row_wait()
        ac_live[mb, j, 0].wait()
        row_mm(mb, 0, a0, n, first)
        y_send(mb, 0)

    def tail_b(l, mb, kind):
        if kind == 'q':
            j, a0, n, first, bs = 0, 0, HALF, True, range(N_Q)
        else:
            j, a0, n, first, bs = N_D - 1, (N_D - 1) * D_CHUNK, D_CHUNK, False, range(N_G - 3, N_G)
        for b in bs:
            a_live[mb, b].wait()
        act_to_core(mb, 1, j, a0, n)
        ac_live[mb, j, 1].wait()
        row_mm(mb, 1, a0, n, first)
        row_done()
        y_send(mb, 1)

    def down_mid(mb, j):
        a0 = j * D_CHUNK
        act_to_core(mb, 0, j, a0, D_CHUNK)
        for b in range(3 * j, 3 * j + 3):
            a_live[mb, b].wait()
        act_to_core(mb, 1, j, a0, D_CHUNK)
        row_wait()
        for xs in range(2):
            ac_live[mb, j, xs].wait()
            row_mm(mb, xs, a0, D_CHUNK, j == 0)
        row_done()

    def update_and_squares(mb):
        r_update(mb)
        norm_squares(mb)

    def finish_out(mb):
        r_update(mb)
        out_send(mb)

    n_steps = len(steps)
    for k, (l, mb, kind, b) in enumerate(steps):
        last = b == (N_Q if kind == 'q' else N_G) - 1
        if kind == 'g' and b % 3 == 2 and not last:
            at(k + 2, down_mid, mb, b // 3)
        if last:
            at(k + 1, tail_a, l, mb, kind)
            at(k + 2, tail_b, l, mb, kind)
            if kind == 'g' and l == n_layers - 1:
                at(k + 3, finish_out, mb)
            else:
                at(k + 3, update_and_squares, mb)
                at(k + 4, norm_apply, mb, 2 * l + 1 if kind == 'q' else 2 * l + 2)
                at(k + 5, norm_finish, mb)
    at(1, norm_squares, 1)
    at(2, norm_apply, 1, 0)
    at(3, norm_finish, 1)
    at(3, swap_gu, 0)
    if n_layers > 1:
        at(2 * N_Q + 7, swap_qkv, 1, False)
        at(2 * N_Q + 12, swap_gu, 1)

    for mb in range(2):
        R[mb] = x_ref[mb].astype(F32)
    norm_squares(0)
    swap_qkv(0, True)
    row_start(0)
    w_start(0)
    norm_apply(0, 0)
    norm_finish(0)
    w_start(1)
    for k in range(n_steps + 4):
        if k < n_steps:
            issue(k)
        if 1 <= k <= n_steps:
            consume(k - 1)
        for f in todo.pop(k, []):
            f()
    assert not todo
    for k in (n_steps - 2, n_steps - 1):
        x_live[k].wait_send()
    for c in o_live:
        c.wait()


def solution(mesh):
    act_spec = P(None, ('rep', 'tok', 'mp'), None)
    seg_spec = P(None, ('rep', 'tok', 'mp'))
    gain_spec = P(None, None)
    head_in = P(None, 'tok', 'mp', None)
    head_out = P(None, 'mp', None, 'tok')
    ffn_in = P(None, 'tok', 'mp')
    ffn_out = P(None, 'mp', 'tok')

    def to_t(v, bits):
        return lax.ppermute(v, 'tok', [(i, i ^ bits) for i in range(4)])

    def device_fn(x_in, seg_ids, g_attn, w_q, w_k, w_v, w_o, g_mlp, w_gate, w_up, w_down):
        n_layers = w_q.shape[0]
        micro_n, loc_len, embed = x_in.shape
        feat, heads, head_dim = w_q.shape[1:]
        t = lax.axis_index('tok')
        m = lax.axis_index('mp')
        core = t % 2
        xpos = t // 2

        seg_all = lax.all_gather(seg_ids, ('tok', 'mp'), axis=1, tiled=True)
        blk_len = 2 * loc_len
        seg_own = lax.dynamic_slice_in_dim(seg_all, xpos * 2 * blk_len, 2 * blk_len, 1).reshape(micro_n, 2, blk_len)
        pos_own = seg_positions(seg_own)
        in_blk = jnp.broadcast_to(jnp.arange(blk_len, dtype=jnp.int32), seg_own.shape)
        blk_id = jnp.broadcast_to(jnp.arange(2, dtype=jnp.int32)[:, None], seg_own.shape)

        def to_rows(v):
            v4 = v.reshape(micro_n, 2, 2, loc_len)
            v4 = jnp.where(m == 0, v4, v4[:, :, ::-1])
            return v4.transpose(0, 2, 1, 3).reshape(micro_n, 2 * blk_len)
        seg_r, pos_r, in_r, blk_r = to_rows(seg_own), to_rows(pos_own), to_rows(in_blk), to_rows(blk_id)

        def eq(v):
            return v[:, :, None] == v[:, None, :]
        allowed = eq(seg_r) & eq(blk_r) & (in_r[:, None, :] <= in_r[:, :, None])
        cos_t, sin_t = rope_tables(pos_r, head_dim)
        cos_f = jnp.concatenate([cos_t, cos_t], axis=-1)
        sin_f = jnp.concatenate([-sin_t, sin_t], axis=-1)

        def piece(k):
            s = lax.dynamic_slice_in_dim(x_in, (t ^ k) * feat, feat, 2)
            return to_t(s, k) if k else s
        p = [piece(k) for k in range(4)]
        lo = jnp.where(core == 0, jnp.stack([p[0], p[1], p[2], p[3]], 1), jnp.stack([p[1], p[0], p[3], p[2]], 1))
        x_rows = lo.reshape(micro_n, 4 * loc_len, feat)

        gains = jnp.stack([g[l] for l in range(n_layers) for g in (g_attn, g_mlp)])
        gains = lax.dynamic_slice_in_dim(gains, t * feat, feat, 1).astype(F32)
        flat_q, flat_k, flat_v = [w.reshape(n_layers, feat, heads * head_dim) for w in (w_q, w_k, w_v)]
        flat_o = w_o.reshape(n_layers, heads * head_dim, feat)

        vm = pl.BlockSpec(memory_space=pltpu.VMEM)
        hb = pl.BlockSpec(memory_space=pltpu.HBM)
        dma = pltpu.SemaphoreType.DMA
        out = pl.pallas_call(
            functools.partial(body, n_layers),
            out_shape=(jax.ShapeDtypeStruct((micro_n, loc_len, embed), F32),
                       jax.ShapeDtypeStruct((n_layers, 3, FEAT, HALF), BF16),
                       jax.ShapeDtypeStruct((n_layers, 2, FEAT, FHALF), BF16)),
            in_specs=[vm] * 5 + [hb] * 7,
            out_specs=(hb, hb, hb),
            scratch_shapes=[
                pltpu.VMEM((2, 256, FEAT), F32),
                pltpu.VMEM((2, 512, FEAT), BF16),
                pltpu.VMEM((2, 512, FEAT), BF16),
                pltpu.VMEM((2, ROWS, SW), F32),
                pltpu.VMEM((2, ROWS, SW), F32),
                pltpu.VMEM((4, ROWS, SW), F32),
                pltpu.VMEM((2, 2, FEAT, SW), BF16),
                pltpu.VMEM((2, HALF, FEAT), BF16),
                pltpu.VMEM((2, 4, ROWS, FHALF), BF16),
                pltpu.VMEM((2, 2, ROWS, FEAT), F32),
                pltpu.VMEM((2, 2, 128, FEAT), F32),
                pltpu.VMEM((2, 256, 128), F32),
                pltpu.VMEM((2, 256, 128), F32),
                pltpu.VMEM((2, 256, 128), F32),
                pltpu.VMEM((2, 256, 128), F32),
                dma((2,)), dma((4,)),
                dma((2, N_G)), dma((2, N_G)),
                dma((2, N_D, 2)), dma((2, N_D, 2)),
                dma((2, 2)), dma((2, 2)),
                dma((2, 2)), dma((2, 2)),
                dma((2, 4)), dma((2, 4)),
                dma((2,)), dma((2,)), dma((2,)), dma((2,)),
                dma((22,)), dma((22,)),
                dma((2, 4)), dma((2, 4)),
                dma((2, 6)), dma((2,)),
            ],
            compiler_params=pltpu.CompilerParams(collective_id=0, has_side_effects=True, vmem_limit_bytes=67043328),
        )(x_rows, cos_f, sin_f, allowed.astype(F32), gains, flat_q, flat_k, flat_v, flat_o, w_gate, w_up, w_down)
        return out[0]

    return jax.shard_map(
        device_fn,
        mesh=mesh,
        in_specs=(act_spec, seg_spec, gain_spec, head_in, head_in, head_in, head_out, gain_spec, ffn_in, ffn_in, ffn_out),
        out_specs=act_spec,
        check_vma=False,
    )
```

```python
import functools

import jax
import jax.numpy as jnp
from jax import lax
from jax.experimental import pallas as pl
from jax.experimental.pallas import tpu as pltpu
from jax.sharding import PartitionSpec as P

NORM_EPS = 1e-5
ROPE_BASE = 10000.0
NEG_BIG = -1e30
F32 = jnp.float32
BF16 = jnp.bfloat16
MESH = pl.DeviceIdType.MESH


def rope_tables(positions, head_dim):
    half_dim = head_dim // 2
    inv_freq = ROPE_BASE ** (-2.0 * jnp.arange(half_dim, dtype=F32) / head_dim)
    angles = positions.astype(F32)[..., None] * inv_freq
    return jnp.cos(angles), jnp.sin(angles)


def mm(a, b):
    return jnp.dot(a, b, preferred_element_type=F32)


FEAT = 1280
EMBED = 5120
HALF = 1280
HEADS = 10
FHALF = 3456
ROWS = 256
QB = 256
GB = 384
SW = 768
N_Q = HALF // QB
N_G = FHALF // GB
D_CHUNK = 3 * GB
N_D = FHALF // D_CHUNK
CB = 256


def body(n_layers, x_ref, cos_ref, sin_ref, mask_ref, gain_ref, wq, wk, wv, wo, wg, wu, wd,
         out_ref, qkvr, gur,
         XB, R, H, HC, XS, XO, XR, W, WR, ACT, PB, YR, SQ, SQC, SQS, SQX,
         xs_s, xr_s, as_s, ar_s, acs_s, acr_s, ys_s, yr_s, hys_s, hyr_s, hcs_s, hcr_s,
         sqcs_s, sqcr_s, sqxs_s, sqxr_s, sws_s, swr_s, os_s, or_s, xbs_s, xbr_s, w_s, wr_s):
    m = lax.axis_index('mp')
    t = lax.axis_index('tok')
    core = lax.rem(t, 2)
    xpos = lax.div(t, 2)
    t_c = xpos * 2 + (1 - core)
    t_x = (1 - xpos) * 2 + core
    t_d = (1 - xpos) * 2 + (1 - core)
    rep = lax.axis_index('rep')
    dev = {'c': (rep, m, t_c), 'x': (rep, m, t_x), 'd': (rep, m, t_d), 'y': (rep, 1 - m, t)}

    barrier = pltpu.get_barrier_semaphore()
    for k in ('c', 'x', 'd', 'y'):
        pl.semaphore_signal(barrier, inc=1, device_id=dev[k], device_id_type=MESH)
    pl.semaphore_wait(barrier, 4)

    def rcopy(src, dst, ss, rs, to):
        return pltpu.make_async_remote_copy(src_ref=src, dst_ref=dst, send_sem=ss, recv_sem=rs,
                                            device_id=dev[to], device_id_type=MESH)

    def al(v, n=128):
        return pl.multiple_of(v, n)

    swaps = {}
    n_sw = [0]

    def swap_start(key, src, dst):
        i = n_sw[0]
        n_sw[0] += 1
        c = rcopy(src, dst, sws_s.at[i], swr_s.at[i], 'c')
        c.start()
        swaps[key] = [c, False]

    def swap_need(key):
        e = swaps[key]
        if not e[1]:
            e[0].wait()
            e[1] = True

    def swap_qkv(l, bs):
        for b in bs:
            for i, w in enumerate((wq, wk, wv)):
                swap_start((l, 'qkv', i, b), w.at[l, pl.ds((1 - core) * HEADS + b * 2, 2)], qkvr.at[l, i, pl.ds(b * 2, 2)])

    def swap_qkv_whole(l):
        for i, w in enumerate((wq, wk, wv)):
            swap_start((l, 'qkv', i), w.at[l, pl.ds((1 - core) * HEADS, HEADS)], qkvr.at[l, i])
            for b in range(N_Q):
                swaps[(l, 'qkv', i, b)] = swaps[(l, 'qkv', i)]

    def swap_gu(l):
        for i, w in enumerate((wg, wu)):
            swap_start((l, 'gu', i), w.at[l, :, pl.ds(al((1 - core) * FHALF), FHALF)], gur.at[l, i])

    steps = []
    for l in range(n_layers):
        for mb in range(2):
            steps += [(l, mb, 'q', b) for b in range(N_Q)]
        for mb in range(2):
            steps += [(l, mb, 'g', b) for b in range(N_G)]

    def w_copies(k):
        l, mb, kind, b = steps[k]
        s = k % 2
        cs = []
        if kind == 'q':
            for i, w in enumerate((wq, wk, wv)):
                for hh in range(2):
                    cols = pl.ds(i * QB + hh * 128, 128)
                    cs.append((w.at[l, core * HEADS + b * 2 + hh], W.at[s, 0, :, cols]))
                    cs.append((qkvr.at[l, i, b * 2 + hh], W.at[s, 1, :, cols]))
        else:
            for i, w in enumerate((wg, wu)):
                cs.append((w.at[l, :, pl.ds(al(core * FHALF + b * GB), GB)], W.at[s, 0, :, pl.ds(i * GB, GB)]))
                cs.append((gur.at[l, i, :, pl.ds(b * GB, GB)], W.at[s, 1, :, pl.ds(i * GB, GB)]))
        return [pltpu.make_async_copy(a, d, w_s.at[s, j]) for j, (a, d) in enumerate(cs)]

    w_live = {}

    def w_start(k):
        if k >= len(steps):
            return
        l, mb, kind, b = steps[k]
        if kind == 'q':
            for i in range(3):
                swap_need((l, 'qkv', i, b))
        else:
            for i in range(2):
                swap_need((l, 'gu', i))
        w_live[k] = w_copies(k)
        for c in w_live[k]:
            c.start()

    x_live = {}

    def issue(k):
        l, mb, kind, b = steps[k]
        s = k % 2
        for c in w_live.pop(k):
            c.wait()
        if k >= 2:
            x_live[k - 2].wait_send()

        def half(row0, dst):
            @pl.loop(0, SW // CB)
            def _(j):
                cols = pl.ds(al(j * CB, CB), CB)
                dst[s, :, cols] = (mm(H[mb, pl.ds(row0, ROWS), :], W[s, 0, :, cols])
                                   + mm(HC[mb, pl.ds(row0, ROWS), :], W[s, 1, :, cols]))
        norm_ready(mb, 1)
        half(ROWS, XS)
        x_live[k] = rcopy(XS.at[s], XR.at[k % 4], xs_s.at[s], xr_s.at[k % 4], 'x')
        x_live[k].start()
        if k == 0:
            w_start(1)
        norm_ready(mb, 0)
        half(0, XO)
        w_start(k + 2)

    a_live = {}

    def consume(k):
        l, mb, kind, b = steps[k]
        s, q = k % 2, k % 4
        x_live[k].wait_recv()
        if kind == 'q':
            cos, sin = cos_ref[mb], sin_ref[mb]
            for hh in range(QB // 128):
                def part(i):
                    c0 = i * QB + hh * 128
                    return XO[s, :, c0:c0 + 128] + XR[q, :, c0:c0 + 128]

                def rope(v):
                    return (v * cos + pltpu.roll(v, 64, 1) * sin).astype(BF16)
                qh, kh, vh = rope(part(0)), rope(part(1)), part(2).astype(BF16)
                sc = lax.dot_general(qh, kh, (((1,), (1,)), ((), ())), preferred_element_type=F32) * (128 ** -0.5)
                sc = jnp.where(mask_ref[mb] > 0.0, sc, NEG_BIG)
                e = jnp.exp(sc - jnp.max(sc, axis=-1, keepdims=True))
                p = (e / jnp.sum(e, axis=-1, keepdims=True)).astype(BF16)
                ACT[mb, 0, :, b * QB + hh * 128:b * QB + hh * 128 + 128] = mm(p, vh).astype(BF16)
            cols = pl.ds(b * QB, QB)
        else:
            g = XO[s, :, :GB] + XR[q, :, :GB]
            u = XO[s, :, GB:] + XR[q, :, GB:]
            ACT[mb, 0, :, b * GB:(b + 1) * GB] = (jax.nn.silu(g) * u).astype(BF16)
            cols = pl.ds(b * GB, GB)
        c = rcopy(ACT.at[mb, 0, :, cols], ACT.at[mb, 1, :, cols], as_s.at[mb, b], ar_s.at[mb, b], 'x')
        c.start()
        a_live[mb, b] = c

    row_seq = []
    for l in range(n_layers):
        row_seq += [(l, mb, 'o', 0) for mb in range(2)] + [(l, mb, 'd', j) for mb in range(2) for j in range(N_D)]
    row_live = {}

    def row_start(i):
        if i >= len(row_seq):
            return
        l, mb, kind, j = row_seq[i]
        if kind == 'o':
            n, src = HALF, lambda c: wo.at[l, pl.ds(al(c * HALF), HALF), :]
        else:
            n, src = D_CHUNK, lambda c: wd.at[l, pl.ds(al(c * FHALF + j * D_CHUNK), D_CHUNK), :]
        row_live[i] = [pltpu.make_async_copy(src(core), WR.at[0, pl.ds(0, n), :], wr_s.at[0]),
                       pltpu.make_async_copy(src(1 - core), WR.at[1, pl.ds(0, n), :], wr_s.at[1])]
        for c in row_live[i]:
            c.start()

    row_at = [0]

    def row_wait():
        for c in row_live.pop(row_at[0]):
            c.wait()

    def row_done():
        row_at[0] += 1
        row_start(row_at[0])

    def row_mm(mb, xs, a0, n, first):
        @pl.loop(0, FEAT // CB)
        def _(j):
            cols = pl.ds(al(j * CB, CB), CB)
            v = (mm(ACT[mb, xs, :, a0:a0 + n], WR[0, :n, cols])
                 + mm(ACT[mb, 2 + xs, :, a0:a0 + n], WR[1, :n, cols]))
            if first:
                PB[mb, xs, :, cols] = v
            else:
                PB[mb, xs, :, cols] += v

    ac_live = {}

    def act_to_core(mb, xs, j, a0, n):
        cols = pl.ds(a0, n)
        c = rcopy(ACT.at[mb, xs, :, cols], ACT.at[mb, 2 + xs, :, cols], acs_s.at[mb, j, xs], acr_s.at[mb, j, xs], 'c')
        c.start()
        ac_live[mb, j, xs] = c

    y_live = {}

    def y_send(mb, xs, hf):
        cols = pl.ds(hf * (FEAT // 2), FEAT // 2)
        c = rcopy(PB.at[mb, xs, pl.ds(128, 128), cols], YR.at[mb, xs, :, cols], ys_s.at[mb, xs, hf], yr_s.at[mb, xs, hf], 'y')
        c.start()
        y_live[mb, xs, hf] = c

    def r_update(mb, xs, hf):
        y_live[mb, xs, hf].wait()
        rows = slice(xs * 128, xs * 128 + 128)
        cols = slice(hf * (FEAT // 2), (hf + 1) * (FEAT // 2))
        R[mb, rows, cols] = R[mb, rows, cols] + (PB[mb, xs, :128, cols] + YR[mb, xs, :, cols])

    n_live = {}

    def norm_squares(mb):
        acc = None
        for j in range(FEAT // 128):
            v = R[mb, :, j * 128:(j + 1) * 128]
            acc = v * v if acc is None else acc + v * v
        SQ[mb] = acc
        c = rcopy(SQ.at[mb], SQC.at[mb], sqcs_s.at[mb], sqcr_s.at[mb], 'c')
        c.start()
        c.wait()
        SQS[mb] = SQ[mb] + SQC[mb]
        c = rcopy(SQS.at[mb], SQX.at[mb], sqxs_s.at[mb], sqxr_s.at[mb], 'x')
        c.start()
        n_live[mb, 'sq'] = c

    def norm_apply(mb, gi):
        n_live[mb, 'sq'].wait()
        for xs in range(2):
            o = 1 - xs
            tot = SQS[mb, xs * 128:(xs + 1) * 128, :] + SQX[mb, o * 128:(o + 1) * 128, :]
            scale = lax.rsqrt(jnp.sum(tot, axis=-1, keepdims=True) / EMBED + NORM_EPS)
            h = R[mb, xs * 128:(xs + 1) * 128, :] * scale * gain_ref[gi:gi + 1, :]
            H[mb, xs * 256:xs * 256 + 128, :] = h.astype(BF16)
        for xs in (1, 0):
            mine, theirs = pl.ds(xs * 256, 128), pl.ds(xs * 256 + 128, 128)
            c = rcopy(H.at[mb, mine, :], H.at[mb, theirs, :], hys_s.at[mb, xs], hyr_s.at[mb, xs], 'y')
            c.start()
            n_live[mb, 'y', xs] = c
        for xs in (1, 0):
            mine = pl.ds(xs * 256, 128)
            c = rcopy(H.at[mb, mine, :], HC.at[mb, mine, :], hcs_s.at[mb, xs], hcr_s.at[mb, xs], 'c')
            c.start()
            n_live[mb, 'c', xs] = c

    def norm_forward(mb, xs):
        if (mb, 'y', xs) in n_live:
            n_live.pop((mb, 'y', xs)).wait()
            theirs = pl.ds(xs * 256 + 128, 128)
            c = rcopy(H.at[mb, theirs, :], HC.at[mb, theirs, :], hcs_s.at[mb, 2 + xs], hcr_s.at[mb, 2 + xs], 'c')
            c.start()
            n_live[mb, 'c', 2 + xs] = c

    def norm_ready(mb, xs):
        norm_forward(mb, xs)
        for i in (xs, 2 + xs):
            if (mb, 'c', i) in n_live:
                n_live.pop((mb, 'c', i)).wait()

    def norm_finish(mb):
        for xs in (1, 0):
            norm_forward(mb, xs)
        for xs in (1, 0):
            norm_ready(mb, xs)

    o_live = []

    def out_send(mb, xs, hf):
        fh = FEAT // 2
        cols = pl.ds(al(t * FEAT + hf * fh), fh)
        for flip in range(2):
            cp = core + flip * (1 - 2 * core)
            src = R.at[mb, pl.ds(al(xs * 128 + cp * 64, 64), 64), pl.ds(hf * fh, fh)]
            to = ('self', 'c', 'x', 'd')[2 * xs + flip]
            i = 2 * xs + flip
            if to == 'self':
                c = pltpu.make_async_copy(src, out_ref.at[mb, :, cols], os_s.at[mb, hf, i])
            else:
                c = rcopy(src, out_ref.at[mb, :, cols], os_s.at[mb, hf, i], or_s.at[mb, hf, i], to)
            c.start()
            o_live.append(c)

    def x_send(mb):
        for i, (k, xs) in enumerate((('x', 1), ('d', 1), ('c', 0), ('self', 0))):
            to_t = {'x': t_x, 'd': t_d, 'c': t_c, 'self': t}[k]
            src = x_ref.at[mb, :, pl.ds(al(to_t * FEAT), FEAT)]
            dst = XB.at[mb, pl.ds(al(xs * 128 + core * 64, 64), 64), :]
            if k == 'self':
                c = pltpu.make_async_copy(src, dst, xbs_s.at[mb, i])
            else:
                c = rcopy(src, dst, xbs_s.at[mb, i], xbr_s.at[mb, i], k)
            c.start()
            n_live[mb, 'xb', i] = c

    def x_take(mb):
        for i in range(4):
            n_live.pop((mb, 'xb', i)).wait()
        R[mb] = XB[mb].astype(F32)

    todo = {}

    def at(k, f, *args):
        todo.setdefault(k, []).append(functools.partial(f, *args))

    def tail_a(l, mb, kind):
        if kind == 'q':
            j, a0, n, first = 0, 0, HALF, True
        else:
            j, a0, n, first = N_D - 1, (N_D - 1) * D_CHUNK, D_CHUNK, False
        act_to_core(mb, 0, j, a0, n)
        row_wait()
        ac_live[mb, j, 0].wait()
        row_mm(mb, 0, a0, n, first)
        y_send(mb, 0, 0)
        if not (l == n_layers - 1 and kind == 'g'):
            y_send(mb, 0, 1)

    def tail_b(l, mb, kind):
        if kind == 'q':
            j, a0, n, first, bs = 0, 0, HALF, True, range(N_Q)
        else:
            j, a0, n, first, bs = N_D - 1, (N_D - 1) * D_CHUNK, D_CHUNK, False, range(N_G - 3, N_G)
        for b in bs:
            a_live[mb, b].wait()
        act_to_core(mb, 1, j, a0, n)
        ac_live[mb, j, 1].wait()
        row_mm(mb, 1, a0, n, first)
        row_done()
        y_send(mb, 1, 0)
        y_send(mb, 1, 1)
        if l == n_layers - 1 and kind == 'g':
            y_send(mb, 0, 1)

    def down_mid(mb, j):
        a0 = j * D_CHUNK
        act_to_core(mb, 0, j, a0, D_CHUNK)
        for b in range(3 * j, 3 * j + 3):
            a_live[mb, b].wait()
        act_to_core(mb, 1, j, a0, D_CHUNK)
        row_wait()
        for xs in range(2):
            ac_live[mb, j, xs].wait()
            row_mm(mb, xs, a0, D_CHUNK, j == 0)
        row_done()

    def update_and_squares(mb):
        for xs in range(2):
            for hf in range(2):
                r_update(mb, xs, hf)
        norm_squares(mb)

    def finish_out(mb):
        for xs, hf in ((1, 0), (1, 1), (0, 0), (0, 1)):
            r_update(mb, xs, hf)
            out_send(mb, xs, hf)

    def first_squares(mb):
        x_take(mb)
        norm_squares(mb)

    n_steps = len(steps)
    for k, (l, mb, kind, b) in enumerate(steps):
        last = b == (N_Q if kind == 'q' else N_G) - 1
        if kind == 'g' and b % 3 == 2 and not last:
            at(k + 2, down_mid, mb, b // 3)
        if last:
            at(k + 1, tail_a, l, mb, kind)
            at(k + 2, tail_b, l, mb, kind)
            if kind == 'g' and l == n_layers - 1:
                at(k + 3, finish_out, mb)
            else:
                at(k + 3, update_and_squares, mb)
                at(k + 4, norm_apply, mb, 2 * l + 1 if kind == 'q' else 2 * l + 2)
                at(k + 5, norm_finish, mb)
    at(1, first_squares, 1)
    at(2, norm_apply, 1, 0)
    at(3, norm_finish, 1)
    at(3, swap_gu, 0)
    if n_layers > 1:
        at(2 * N_Q + 7, swap_qkv_whole, 1)
        at(2 * N_Q + 12, swap_gu, 1)

    x_send(0)
    swap_qkv(0, (0,))
    row_start(0)
    first_squares(0)
    x_send(1)
    w_start(0)
    norm_apply(0, 0)
    swap_qkv(0, range(1, N_Q))
    for k in range(n_steps + 4):
        if k < n_steps:
            issue(k)
        if 1 <= k <= n_steps:
            consume(k - 1)
        for f in todo.pop(k, []):
            f()
    assert not todo
    for k in (n_steps - 2, n_steps - 1):
        x_live[k].wait_send()
    for c in o_live:
        c.wait()


def solution(mesh):
    act_spec = P(None, ('rep', 'tok', 'mp'), None)
    seg_spec = P(None, ('rep', 'tok', 'mp'))
    gain_spec = P(None, None)
    head_in = P(None, 'tok', 'mp', None)
    head_out = P(None, 'mp', None, 'tok')
    ffn_in = P(None, 'tok', 'mp')
    ffn_out = P(None, 'mp', 'tok')

    def device_fn(x_in, seg_ids, g_attn, w_q, w_k, w_v, w_o, g_mlp, w_gate, w_up, w_down):
        n_layers = w_q.shape[0]
        micro_n, loc_len, embed = x_in.shape
        feat, heads, head_dim = w_q.shape[1:]
        t = lax.axis_index('tok')
        m = lax.axis_index('mp')
        core = t % 2
        xpos = t // 2

        seg_y = lax.ppermute(seg_ids, 'mp', [(0, 1), (1, 0)])
        seg_c = lax.ppermute(seg_ids, 'tok', [(i, i ^ 1) for i in range(4)])
        seg_yc = lax.ppermute(seg_ids, ('mp', 'tok'), [(i, i ^ 5) for i in range(8)])
        mine, theirs = jnp.stack([seg_ids, seg_y], 1), jnp.stack([seg_c, seg_yc], 1)
        seg_r = jnp.where(core == 0, jnp.stack([mine, theirs], 2), jnp.stack([theirs, mine], 2)).reshape(micro_n, 4 * loc_len)
        row = jnp.arange(4 * loc_len, dtype=jnp.int32)
        in_r = ((row // (2 * loc_len)) ^ m) * loc_len + row % loc_len
        blk_r = (row // loc_len) % 2
        allowed = ((seg_r[:, :, None] == seg_r[:, None, :]) & (blk_r[:, None] == blk_r[None, :])
                   & (in_r[None, :] <= in_r[:, None]))
        pos_r = jnp.sum(allowed.astype(jnp.int32), axis=-1) - 1
        cos_t, sin_t = rope_tables(pos_r, head_dim)
        cos_f = jnp.concatenate([cos_t, cos_t], axis=-1)
        sin_f = jnp.concatenate([-sin_t, sin_t], axis=-1)

        gains = jnp.stack([g[l] for l in range(n_layers) for g in (g_attn, g_mlp)])
        gains = lax.dynamic_slice_in_dim(gains, t * feat, feat, 1).astype(F32)
        by_head = [w.transpose(0, 2, 1, 3) for w in (w_q, w_k, w_v)]
        flat_o = w_o.reshape(n_layers, heads * head_dim, feat)

        vm = pl.BlockSpec(memory_space=pltpu.VMEM)
        hb = pl.BlockSpec(memory_space=pltpu.HBM)
        dma = pltpu.SemaphoreType.DMA
        out = pl.pallas_call(
            functools.partial(body, n_layers),
            out_shape=(jax.ShapeDtypeStruct((micro_n, loc_len, embed), F32),
                       jax.ShapeDtypeStruct((n_layers, 3, HEADS, FEAT, 128), BF16),
                       jax.ShapeDtypeStruct((n_layers, 2, FEAT, FHALF), BF16)),
            in_specs=[hb] + [vm] * 4 + [hb] * 7,
            out_specs=(hb, hb, hb),
            scratch_shapes=[
                pltpu.VMEM((2, 256, FEAT), BF16),
                pltpu.VMEM((2, 256, FEAT), F32),
                pltpu.VMEM((2, 512, FEAT), BF16),
                pltpu.VMEM((2, 512, FEAT), BF16),
                pltpu.VMEM((2, ROWS, SW), F32),
                pltpu.VMEM((2, ROWS, SW), F32),
                pltpu.VMEM((4, ROWS, SW), F32),
                pltpu.VMEM((2, 2, FEAT, SW), BF16),
                pltpu.VMEM((2, HALF, FEAT), BF16),
                pltpu.VMEM((2, 4, ROWS, FHALF), BF16),
                pltpu.VMEM((2, 2, ROWS, FEAT), F32),
                pltpu.VMEM((2, 2, 128, FEAT), F32),
                pltpu.VMEM((2, 256, 128), F32),
                pltpu.VMEM((2, 256, 128), F32),
                pltpu.VMEM((2, 256, 128), F32),
                pltpu.VMEM((2, 256, 128), F32),
                dma((2,)), dma((4,)),
                dma((2, N_G)), dma((2, N_G)),
                dma((2, N_D, 2)), dma((2, N_D, 2)),
                dma((2, 2, 2)), dma((2, 2, 2)),
                dma((2, 2)), dma((2, 2)),
                dma((2, 4)), dma((2, 4)),
                dma((2,)), dma((2,)), dma((2,)), dma((2,)),
                dma((22,)), dma((22,)),
                dma((2, 2, 4)), dma((2, 2, 4)),
                dma((2, 4)), dma((2, 4)),
                dma((2, 12)), dma((2,)),
            ],
            compiler_params=pltpu.CompilerParams(collective_id=0, has_side_effects=True, vmem_limit_bytes=67043328),
        )(x_in, cos_f, sin_f, allowed.astype(F32), gains, *by_head, flat_o, w_gate, w_up, w_down)
        return out[0]

    return jax.shard_map(
        device_fn,
        mesh=mesh,
        in_specs=(act_spec, seg_spec, gain_spec, head_in, head_in, head_in, head_out, gain_spec, ffn_in, ffn_in, ffn_out),
        out_specs=act_spec,
        check_vma=False,
    )
```

```python
import functools

import jax
import jax.numpy as jnp
import numpy as np
from jax import lax
from jax.experimental import pallas as pl
from jax.experimental.pallas import tpu as pltpu
from jax.sharding import PartitionSpec as P

NORM_EPS = 1e-5
ROPE_BASE = 10000.0
NEG_BIG = -1e30
F32 = jnp.float32
BF16 = jnp.bfloat16
MESH = pl.DeviceIdType.MESH


def rope_rows(n_pos, head_dim):
    half_dim = head_dim // 2
    inv_freq = np.float32(ROPE_BASE) ** (np.float32(-2.0) * np.arange(half_dim, dtype=np.float32) / np.float32(head_dim))
    angles = np.arange(n_pos, dtype=np.float32)[:, None] * inv_freq.astype(np.float32)
    cos_t, sin_t = np.cos(angles), np.sin(angles)
    return np.concatenate([cos_t, cos_t], axis=-1), np.concatenate([-sin_t, sin_t], axis=-1)


def mm(a, b):
    return jnp.dot(a, b, preferred_element_type=F32)


FEAT = 1280
EMBED = 5120
HALF = 1280
HEADS = 10
FHALF = 3456
ROWS = 256
QB = 256
GB = 384
SW = 768
N_Q = HALF // QB
N_G = FHALF // GB
D_CHUNK = 3 * GB
N_D = FHALF // D_CHUNK
CB = 256


def body(n_layers, x_ref, seg_ref, ctab_ref, stab_ref, ga_ref, gm_ref, wq, wk, wv, wo, wg, wu, wd,
         out_ref, qkvr, gur,
         SEG, cos_ref, sin_ref, mask_ref, XB, R, H, HC, XS, XO, XR, W, WR, ACT, PB, YR, SQ, SQC, SQS, SQX,
         xs_s, xr_s, as_s, ar_s, acs_s, acr_s, ys_s, yr_s, hys_s, hyr_s, hcs_s, hcr_s,
         sqcs_s, sqcr_s, sqxs_s, sqxr_s, sws_s, swr_s, os_s, or_s, xbs_s, xbr_s, sgs_s, sgr_s, w_s, wr_s):
    m = lax.axis_index('mp')
    t = lax.axis_index('tok')
    core = lax.rem(t, 2)
    xpos = lax.div(t, 2)
    t_c = xpos * 2 + (1 - core)
    t_x = (1 - xpos) * 2 + core
    t_d = (1 - xpos) * 2 + (1 - core)
    rep = lax.axis_index('rep')
    dev = {'c': (rep, m, t_c), 'x': (rep, m, t_x), 'd': (rep, m, t_d), 'y': (rep, 1 - m, t), 'yc': (rep, 1 - m, t_c)}

    barrier = pltpu.get_barrier_semaphore()
    for k in ('c', 'x', 'd', 'y', 'yc'):
        pl.semaphore_signal(barrier, inc=1, device_id=dev[k], device_id_type=MESH)
    pl.semaphore_wait(barrier, 5)

    def rcopy(src, dst, ss, rs, to):
        return pltpu.make_async_remote_copy(src_ref=src, dst_ref=dst, send_sem=ss, recv_sem=rs,
                                            device_id=dev[to], device_id_type=MESH)

    def al(v, n=128):
        return pl.multiple_of(v, n)

    swaps = {}
    n_sw = [0]

    def swap_start(key, src, dst):
        i = n_sw[0]
        n_sw[0] += 1
        c = rcopy(src, dst, sws_s.at[i], swr_s.at[i], 'c')
        c.start()
        swaps[key] = [c, False]

    def swap_need(key):
        e = swaps[key]
        if not e[1]:
            e[0].wait()
            e[1] = True

    def swap_qkv(l, bs):
        for b in bs:
            for i, w in enumerate((wq, wk, wv)):
                swap_start((l, 'qkv', i, b), w.at[l, pl.ds((1 - core) * HEADS + b * 2, 2)], qkvr.at[l, i, pl.ds(b * 2, 2)])

    def swap_qkv_whole(l):
        for i, w in enumerate((wq, wk, wv)):
            swap_start((l, 'qkv', i), w.at[l, pl.ds((1 - core) * HEADS, HEADS)], qkvr.at[l, i])
            for b in range(N_Q):
                swaps[(l, 'qkv', i, b)] = swaps[(l, 'qkv', i)]

    def swap_gu(l):
        for i, w in enumerate((wg, wu)):
            swap_start((l, 'gu', i), w.at[l, :, pl.ds(al((1 - core) * FHALF), FHALF)], gur.at[l, i])

    steps = []
    for l in range(n_layers):
        for mb in range(2):
            steps += [(l, mb, 'q', b) for b in range(N_Q)]
        for mb in range(2):
            steps += [(l, mb, 'g', b) for b in range(N_G)]

    def w_copies(k):
        l, mb, kind, b = steps[k]
        s = k % 2
        cs = []
        if kind == 'q':
            for i, w in enumerate((wq, wk, wv)):
                for hh in range(2):
                    cols = pl.ds(i * QB + hh * 128, 128)
                    cs.append((w.at[l, core * HEADS + b * 2 + hh], W.at[s, 0, :, cols]))
                    cs.append((qkvr.at[l, i, b * 2 + hh], W.at[s, 1, :, cols]))
        else:
            for i, w in enumerate((wg, wu)):
                cs.append((w.at[l, :, pl.ds(al(core * FHALF + b * GB), GB)], W.at[s, 0, :, pl.ds(i * GB, GB)]))
                cs.append((gur.at[l, i, :, pl.ds(b * GB, GB)], W.at[s, 1, :, pl.ds(i * GB, GB)]))
        return [pltpu.make_async_copy(a, d, w_s.at[s, j]) for j, (a, d) in enumerate(cs)]

    w_live = {}

    def w_start(k):
        if k >= len(steps):
            return
        l, mb, kind, b = steps[k]
        if kind == 'q':
            for i in range(3):
                swap_need((l, 'qkv', i, b))
        else:
            for i in range(2):
                swap_need((l, 'gu', i))
        w_live[k] = w_copies(k)
        for c in w_live[k]:
            c.start()

    x_live = {}

    def issue(k):
        l, mb, kind, b = steps[k]
        s = k % 2
        for c in w_live.pop(k):
            c.wait()
        if k >= 2:
            x_live[k - 2].wait_send()

        def half(row0, dst):
            @pl.loop(0, SW // CB)
            def _(j):
                cols = pl.ds(al(j * CB, CB), CB)
                dst[s, :, cols] = (mm(H[mb, pl.ds(row0, ROWS), :], W[s, 0, :, cols])
                                   + mm(HC[mb, pl.ds(row0, ROWS), :], W[s, 1, :, cols]))
        norm_ready(mb, 1)
        half(ROWS, XS)
        x_live[k] = rcopy(XS.at[s], XR.at[k % 4], xs_s.at[s], xr_s.at[k % 4], 'x')
        x_live[k].start()
        if k == 0:
            w_start(1)
        norm_ready(mb, 0)
        half(0, XO)
        w_start(k + 2)

    a_live = {}

    def consume(k):
        l, mb, kind, b = steps[k]
        s, q = k % 2, k % 4
        x_live[k].wait_recv()
        if kind == 'q':
            cos, sin = cos_ref[mb], sin_ref[mb]
            for hh in range(QB // 128):
                def part(i):
                    c0 = i * QB + hh * 128
                    return XO[s, :, c0:c0 + 128] + XR[q, :, c0:c0 + 128]

                def rope(v):
                    return (v * cos + pltpu.roll(v, 64, 1) * sin).astype(BF16)
                qh, kh, vh = rope(part(0)), rope(part(1)), part(2).astype(BF16)
                sc = lax.dot_general(qh, kh, (((1,), (1,)), ((), ())), preferred_element_type=F32) * (128 ** -0.5)
                sc = jnp.where(mask_ref[mb] > 0.0, sc, NEG_BIG)
                e = jnp.exp(sc - jnp.max(sc, axis=-1, keepdims=True))
                p = (e / jnp.sum(e, axis=-1, keepdims=True)).astype(BF16)
                ACT[mb, 0, :, b * QB + hh * 128:b * QB + hh * 128 + 128] = mm(p, vh).astype(BF16)
            cols = pl.ds(b * QB, QB)
        else:
            g = XO[s, :, :GB] + XR[q, :, :GB]
            u = XO[s, :, GB:] + XR[q, :, GB:]
            ACT[mb, 0, :, b * GB:(b + 1) * GB] = (jax.nn.silu(g) * u).astype(BF16)
            cols = pl.ds(b * GB, GB)
        c = rcopy(ACT.at[mb, 0, :, cols], ACT.at[mb, 1, :, cols], as_s.at[mb, b], ar_s.at[mb, b], 'x')
        c.start()
        a_live[mb, b] = c

    row_seq = []
    for l in range(n_layers):
        row_seq += [(l, mb, 'o', 0) for mb in range(2)] + [(l, mb, 'd', j) for mb in range(2) for j in range(N_D)]
    row_live = {}

    def row_start(i):
        if i >= len(row_seq):
            return
        l, mb, kind, j = row_seq[i]
        if kind == 'o':
            n, src = HALF, lambda c: wo.at[l, pl.ds(al(c * HALF), HALF), :]
        else:
            n, src = D_CHUNK, lambda c: wd.at[l, pl.ds(al(c * FHALF + j * D_CHUNK), D_CHUNK), :]
        row_live[i] = [pltpu.make_async_copy(src(core), WR.at[0, pl.ds(0, n), :], wr_s.at[0]),
                       pltpu.make_async_copy(src(1 - core), WR.at[1, pl.ds(0, n), :], wr_s.at[1])]
        for c in row_live[i]:
            c.start()

    row_at = [0]

    def row_wait():
        for c in row_live.pop(row_at[0]):
            c.wait()

    def row_done():
        row_at[0] += 1
        row_start(row_at[0])

    def row_mm(mb, xs, a0, n, first):
        @pl.loop(0, FEAT // CB)
        def _(j):
            cols = pl.ds(al(j * CB, CB), CB)
            v = (mm(ACT[mb, xs, :, a0:a0 + n], WR[0, :n, cols])
                 + mm(ACT[mb, 2 + xs, :, a0:a0 + n], WR[1, :n, cols]))
            if first:
                PB[mb, xs, :, cols] = v
            else:
                PB[mb, xs, :, cols] += v

    ac_live = {}

    def act_to_core(mb, xs, j, a0, n):
        cols = pl.ds(a0, n)
        c = rcopy(ACT.at[mb, xs, :, cols], ACT.at[mb, 2 + xs, :, cols], acs_s.at[mb, j, xs], acr_s.at[mb, j, xs], 'c')
        c.start()
        ac_live[mb, j, xs] = c

    y_live = {}

    def y_send(mb, xs, hf):
        cols = pl.ds(hf * (FEAT // 2), FEAT // 2)
        c = rcopy(PB.at[mb, xs, pl.ds(128, 128), cols], YR.at[mb, xs, :, cols], ys_s.at[mb, xs, hf], yr_s.at[mb, xs, hf], 'y')
        c.start()
        y_live[mb, xs, hf] = c

    def r_update(mb, xs, hf):
        y_live[mb, xs, hf].wait()
        rows = slice(xs * 128, xs * 128 + 128)
        cols = slice(hf * (FEAT // 2), (hf + 1) * (FEAT // 2))
        R[mb, rows, cols] = R[mb, rows, cols] + (PB[mb, xs, :128, cols] + YR[mb, xs, :, cols])

    n_live = {}

    def norm_squares(mb):
        acc = None
        for j in range(FEAT // 128):
            v = R[mb, :, j * 128:(j + 1) * 128]
            acc = v * v if acc is None else acc + v * v
        SQ[mb] = jnp.broadcast_to(jnp.sum(acc.T, axis=0, keepdims=True), (8, ROWS))
        c = rcopy(SQ.at[mb], SQC.at[mb], sqcs_s.at[mb], sqcr_s.at[mb], 'c')
        c.start()
        c.wait()
        SQS[mb] = SQ[mb] + SQC[mb]
        c = rcopy(SQS.at[mb], SQX.at[mb], sqxs_s.at[mb], sqxr_s.at[mb], 'x')
        c.start()
        n_live[mb, 'sq'] = c

    def norm_apply(mb, gi):
        n_live[mb, 'sq'].wait()
        g_ref = gm_ref if gi % 2 else ga_ref
        gain = g_ref[gi // 2:gi // 2 + 1, pl.ds(al(t * FEAT), FEAT)].astype(F32)
        for xs in range(2):
            o = 1 - xs
            tot = SQS[mb, 0:1, xs * 128:(xs + 1) * 128] + SQX[mb, 0:1, o * 128:(o + 1) * 128]
            scale = jnp.broadcast_to(lax.rsqrt(tot / EMBED + NORM_EPS), (128, 128)).T[:, 0:1]
            h = R[mb, xs * 128:(xs + 1) * 128, :] * scale * gain
            H[mb, xs * 256:xs * 256 + 128, :] = h.astype(BF16)
        for xs in (1, 0):
            mine, theirs = pl.ds(xs * 256, 128), pl.ds(xs * 256 + 128, 128)
            c = rcopy(H.at[mb, mine, :], H.at[mb, theirs, :], hys_s.at[mb, xs], hyr_s.at[mb, xs], 'y')
            c.start()
            n_live[mb, 'y', xs] = c
        for xs in (1, 0):
            mine = pl.ds(xs * 256, 128)
            c = rcopy(H.at[mb, mine, :], HC.at[mb, mine, :], hcs_s.at[mb, xs], hcr_s.at[mb, xs], 'c')
            c.start()
            n_live[mb, 'c', xs] = c

    def norm_forward(mb, xs):
        if (mb, 'y', xs) in n_live:
            n_live.pop((mb, 'y', xs)).wait()
            theirs = pl.ds(xs * 256 + 128, 128)
            c = rcopy(H.at[mb, theirs, :], HC.at[mb, theirs, :], hcs_s.at[mb, 2 + xs], hcr_s.at[mb, 2 + xs], 'c')
            c.start()
            n_live[mb, 'c', 2 + xs] = c

    def norm_ready(mb, xs):
        norm_forward(mb, xs)
        for i in (xs, 2 + xs):
            if (mb, 'c', i) in n_live:
                n_live.pop((mb, 'c', i)).wait()

    def norm_finish(mb):
        for xs in (1, 0):
            norm_forward(mb, xs)
        for xs in (1, 0):
            norm_ready(mb, xs)

    o_live = []

    def out_send(mb, xs, hf):
        fh = FEAT // 2
        cols = pl.ds(al(t * FEAT + hf * fh), fh)
        for flip in range(2):
            cp = core + flip * (1 - 2 * core)
            src = R.at[mb, pl.ds(al(xs * 128 + cp * 64, 64), 64), pl.ds(hf * fh, fh)]
            to = ('self', 'c', 'x', 'd')[2 * xs + flip]
            i = 2 * xs + flip
            if to == 'self':
                c = pltpu.make_async_copy(src, out_ref.at[mb, :, cols], os_s.at[mb, hf, i])
            else:
                c = rcopy(src, out_ref.at[mb, :, cols], os_s.at[mb, hf, i], or_s.at[mb, hf, i], to)
            c.start()
            o_live.append(c)

    def x_send(mb):
        for i, (k, xs) in enumerate((('x', 1), ('d', 1), ('c', 0), ('self', 0))):
            to_t = {'x': t_x, 'd': t_d, 'c': t_c, 'self': t}[k]
            src = x_ref.at[mb, :, pl.ds(al(to_t * FEAT), FEAT)]
            dst = XB.at[mb, pl.ds(al(xs * 128 + core * 64, 64), 64), :]
            if k == 'self':
                c = pltpu.make_async_copy(src, dst, xbs_s.at[mb, i])
            else:
                c = rcopy(src, dst, xbs_s.at[mb, i], xbr_s.at[mb, i], k)
            c.start()
            n_live[mb, 'xb', i] = c

    def x_take(mb):
        for i in range(4):
            n_live.pop((mb, 'xb', i)).wait()
        R[mb] = XB[mb].astype(F32)

    def seg_send(mb):
        for i, (k, mm_half) in enumerate((('y', 1), ('yc', 1), ('c', 0), ('self', 0))):
            dst = SEG.at[mb, pl.ds(al(mm_half * 128 + core * 64, 64), 64), :]
            if k == 'self':
                c = pltpu.make_async_copy(seg_ref.at[mb], dst, sgs_s.at[mb, i])
            else:
                c = rcopy(seg_ref.at[mb], dst, sgs_s.at[mb, i], sgr_s.at[mb, i], k)
            c.start()
            n_live[mb, 'seg', i] = c

    def tables(mb):
        for i in range(4):
            n_live.pop((mb, 'seg', i)).wait()
        seg = SEG[mb]
        same = None
        for v in ((seg >> 12).astype(F32), (seg & 4095).astype(F32)):
            e = v[:, 0:1] == v.T[0:1, :]
            same = e if same is None else same & e
        r = lax.broadcasted_iota(jnp.int32, (ROWS, ROWS), 0)
        c = lax.broadcasted_iota(jnp.int32, (ROWS, ROWS), 1)

        def place(v):
            return ((v >> 7) ^ m) * 64 + (v & 63)
        same = same & (((r >> 6) & 1) == ((c >> 6) & 1)) & (place(c) <= place(r))
        allowed = jnp.where(same, 1.0, 0.0)
        mask_ref[mb] = allowed
        pos = jnp.sum(allowed, axis=-1, keepdims=True) - 1.0
        lane = lax.broadcasted_iota(jnp.int32, (ROWS, 128), 1).astype(F32)
        pick = jnp.where(lane == pos, 1.0, 0.0)
        for tab, dst in ((ctab_ref, cos_ref), (stab_ref, sin_ref)):
            dst[mb] = jnp.dot(pick, tab[...], preferred_element_type=F32, precision=lax.Precision.HIGHEST)

    todo = {}

    early = {}

    def at(k, f, *args):
        todo.setdefault(k, []).append(functools.partial(f, *args))

    def before(k, f, *args):
        early.setdefault(k, []).append(functools.partial(f, *args))

    def tail_a(l, mb, kind):
        if kind == 'q':
            j, a0, n, first = 0, 0, HALF, True
        else:
            j, a0, n, first = N_D - 1, (N_D - 1) * D_CHUNK, D_CHUNK, False
        act_to_core(mb, 0, j, a0, n)
        row_wait()
        ac_live[mb, j, 0].wait()
        row_mm(mb, 0, a0, n, first)
        y_send(mb, 0, 0)
        if not (l == n_layers - 1 and kind == 'g'):
            y_send(mb, 0, 1)

    def tail_b(l, mb, kind):
        if kind == 'q':
            j, a0, n, first, bs = 0, 0, HALF, True, range(N_Q)
        else:
            j, a0, n, first, bs = N_D - 1, (N_D - 1) * D_CHUNK, D_CHUNK, False, range(N_G - 3, N_G)
        for b in bs:
            a_live[mb, b].wait()
        act_to_core(mb, 1, j, a0, n)
        ac_live[mb, j, 1].wait()
        row_mm(mb, 1, a0, n, first)
        row_done()
        y_send(mb, 1, 0)
        y_send(mb, 1, 1)
        if l == n_layers - 1 and kind == 'g':
            y_send(mb, 0, 1)

    def down_mid(mb, j):
        a0 = j * D_CHUNK
        act_to_core(mb, 0, j, a0, D_CHUNK)
        for b in range(3 * j, 3 * j + 3):
            a_live[mb, b].wait()
        act_to_core(mb, 1, j, a0, D_CHUNK)
        row_wait()
        for xs in range(2):
            ac_live[mb, j, xs].wait()
            row_mm(mb, xs, a0, D_CHUNK, j == 0)
        row_done()

    def update_and_squares(mb):
        for xs in range(2):
            for hf in range(2):
                r_update(mb, xs, hf)
        norm_squares(mb)

    pieces = ((1, 0), (1, 1), (0, 0), (0, 1))

    def finish(mb):
        for xs, hf in pieces:
            r_update(mb, xs, hf)

    def send_finished(mb):
        for xs, hf in pieces:
            out_send(mb, xs, hf)

    def finish_out(mb):
        for xs, hf in pieces:
            r_update(mb, xs, hf)
            out_send(mb, xs, hf)

    def first_squares(mb):
        x_take(mb)
        norm_squares(mb)

    n_steps = len(steps)
    at(n_steps, send_finished, 0)
    for k, (l, mb, kind, b) in enumerate(steps):
        last = b == (N_Q if kind == 'q' else N_G) - 1
        if kind == 'g' and b % 3 == 2 and not last:
            before(k + 3, down_mid, mb, b // 3)
        if last:
            before(k + 2, tail_a, l, mb, kind)
            before(k + 3, tail_b, l, mb, kind)
            if kind == 'g' and l == n_layers - 1:
                at(k + 3, finish if mb == 0 else finish_out, mb)
            else:
                at(k + 3, update_and_squares, mb)
                at(k + 4, norm_apply, mb, 2 * l + 1 if kind == 'q' else 2 * l + 2)
                at(k + 5, norm_finish, mb)
    at(0, tables, 0)
    at(1, first_squares, 1)
    at(4, tables, 1)
    at(2, norm_apply, 1, 0)
    at(3, norm_finish, 1)
    at(3, swap_gu, 0)
    if n_layers > 1:
        at(2 * N_Q + 7, swap_qkv_whole, 1)
        at(2 * N_Q + 12, swap_gu, 1)

    x_send(0)
    for mb in range(2):
        seg_send(mb)
    swap_qkv(0, (0,))
    row_start(0)
    first_squares(0)
    x_send(1)
    w_start(0)
    norm_apply(0, 0)
    swap_qkv(0, range(1, N_Q))
    for k in range(n_steps + 4):
        if k < n_steps:
            issue(k)
        for f in early.pop(k, []):
            f()
        if 1 <= k <= n_steps:
            consume(k - 1)
        for f in todo.pop(k, []):
            f()
    assert not todo and not early
    for k in (n_steps - 2, n_steps - 1):
        x_live[k].wait_send()
    for c in o_live:
        c.wait()


def solution(mesh):
    act_spec = P(None, ('rep', 'tok', 'mp'), None)
    seg_spec = P(None, ('rep', 'tok', 'mp'))
    gain_spec = P(None, None)
    head_in = P(None, 'tok', 'mp', None)
    head_out = P(None, 'mp', None, 'tok')
    ffn_in = P(None, 'tok', 'mp')
    ffn_out = P(None, 'mp', 'tok')

    def device_fn(x_in, seg_ids, g_attn, w_q, w_k, w_v, w_o, g_mlp, w_gate, w_up, w_down):
        n_layers = w_q.shape[0]
        micro_n, loc_len, embed = x_in.shape
        feat, heads, head_dim = w_q.shape[1:]
        seg_b = jnp.broadcast_to(seg_ids[:, :, None], (micro_n, loc_len, 128))
        cos_rows, sin_rows = rope_rows(2 * loc_len, head_dim)
        by_head = [w.transpose(0, 2, 1, 3) for w in (w_q, w_k, w_v)]
        flat_o = w_o.reshape(n_layers, heads * head_dim, feat)

        vm = pl.BlockSpec(memory_space=pltpu.VMEM)
        hb = pl.BlockSpec(memory_space=pltpu.HBM)
        dma = pltpu.SemaphoreType.DMA
        out = pl.pallas_call(
            functools.partial(body, n_layers),
            out_shape=(jax.ShapeDtypeStruct((micro_n, loc_len, embed), F32),
                       jax.ShapeDtypeStruct((n_layers, 3, HEADS, FEAT, 128), BF16),
                       jax.ShapeDtypeStruct((n_layers, 2, FEAT, FHALF), BF16)),
            in_specs=[hb] * 2 + [vm] * 4 + [hb] * 7,
            out_specs=(hb, hb, hb),
            scratch_shapes=[
                pltpu.VMEM((2, ROWS, 128), jnp.int32),
                pltpu.VMEM((2, ROWS, 128), F32),
                pltpu.VMEM((2, ROWS, 128), F32),
                pltpu.VMEM((2, ROWS, ROWS), F32),
                pltpu.VMEM((2, 256, FEAT), BF16),
                pltpu.VMEM((2, 256, FEAT), F32),
                pltpu.VMEM((2, 512, FEAT), BF16),
                pltpu.VMEM((2, 512, FEAT), BF16),
                pltpu.VMEM((2, ROWS, SW), F32),
                pltpu.VMEM((2, ROWS, SW), F32),
                pltpu.VMEM((4, ROWS, SW), F32),
                pltpu.VMEM((2, 2, FEAT, SW), BF16),
                pltpu.VMEM((2, HALF, FEAT), BF16),
                pltpu.VMEM((2, 4, ROWS, FHALF), BF16),
                pltpu.VMEM((2, 2, ROWS, FEAT), F32),
                pltpu.VMEM((2, 2, 128, FEAT), F32),
                pltpu.VMEM((2, 8, ROWS), F32),
                pltpu.VMEM((2, 8, ROWS), F32),
                pltpu.VMEM((2, 8, ROWS), F32),
                pltpu.VMEM((2, 8, ROWS), F32),
                dma((2,)), dma((4,)),
                dma((2, N_G)), dma((2, N_G)),
                dma((2, N_D, 2)), dma((2, N_D, 2)),
                dma((2, 2, 2)), dma((2, 2, 2)),
                dma((2, 2)), dma((2, 2)),
                dma((2, 4)), dma((2, 4)),
                dma((2,)), dma((2,)), dma((2,)), dma((2,)),
                dma((22,)), dma((22,)),
                dma((2, 2, 4)), dma((2, 2, 4)),
                dma((2, 4)), dma((2, 4)),
                dma((2, 4)), dma((2, 4)),
                dma((2, 12)), dma((2,)),
            ],
            compiler_params=pltpu.CompilerParams(collective_id=0, has_side_effects=True, vmem_limit_bytes=67043328),
        )(x_in, seg_b, cos_rows, sin_rows, g_attn, g_mlp, *by_head, flat_o, w_gate, w_up, w_down)
        return out[0]

    return jax.shard_map(
        device_fn,
        mesh=mesh,
        in_specs=(act_spec, seg_spec, gain_spec, head_in, head_in, head_in, head_out, gain_spec, ffn_in, ffn_in, ffn_out),
        out_specs=act_spec,
        check_vma=False,
    )
```

```python
import functools

import jax
import jax.numpy as jnp
import numpy as np
from jax import lax
from jax.experimental import pallas as pl
from jax.experimental.pallas import tpu as pltpu
from jax.sharding import PartitionSpec as P

NORM_EPS = 1e-5
ROPE_BASE = 10000.0
NEG_BIG = -1e30
F32 = jnp.float32
BF16 = jnp.bfloat16
MESH = pl.DeviceIdType.MESH


def rope_rows(n_pos, head_dim):
    half_dim = head_dim // 2
    inv_freq = np.float32(ROPE_BASE) ** (np.float32(-2.0) * np.arange(half_dim, dtype=np.float32) / np.float32(head_dim))
    angles = np.arange(n_pos, dtype=np.float32)[:, None] * inv_freq.astype(np.float32)
    cos_t, sin_t = np.cos(angles), np.sin(angles)
    return np.concatenate([cos_t, cos_t], axis=-1), np.concatenate([-sin_t, sin_t], axis=-1)


def mm(a, b):
    return jnp.dot(a, b, preferred_element_type=F32)


FEAT = 1280
EMBED = 5120
HALF = 1280
HEADS = 10
FHALF = 3456
ROWS = 256
QB = 256
GB = 384
SW = 768
N_Q = HALF // QB
N_G = FHALF // GB
D_CHUNK = 3 * GB
N_D = FHALF // D_CHUNK
CB = 256


def body(n_layers, x_ref, seg_ref, ctab_ref, stab_ref, ga_ref, gm_ref, wq, wk, wv, wo, wg, wu, wd,
         out_ref, qkvr, gur,
         SEG, cos_ref, sin_ref, mask_ref, XB, R, H, HC, XP, XR, W, WR, ACT, PB, YR, SQ, SQC, SQS, SQX,
         xs_s, xr_s, as_s, ar_s, acs_s, acr_s, ys_s, yr_s, hys_s, hyr_s, hcs_s, hcr_s,
         sqcs_s, sqcr_s, sqxs_s, sqxr_s, sws_s, swr_s, os_s, or_s, xbs_s, xbr_s, sgs_s, sgr_s, w_s, wr_s):
    m = lax.axis_index('mp')
    t = lax.axis_index('tok')
    core = lax.rem(t, 2)
    xpos = lax.div(t, 2)
    t_c = xpos * 2 + (1 - core)
    t_x = (1 - xpos) * 2 + core
    t_d = (1 - xpos) * 2 + (1 - core)
    rep = lax.axis_index('rep')
    dev = {'c': (rep, m, t_c), 'x': (rep, m, t_x), 'd': (rep, m, t_d), 'y': (rep, 1 - m, t), 'yc': (rep, 1 - m, t_c)}

    barrier = pltpu.get_barrier_semaphore()
    for k in ('c', 'x', 'd', 'y', 'yc'):
        pl.semaphore_signal(barrier, inc=1, device_id=dev[k], device_id_type=MESH)
    pl.semaphore_wait(barrier, 5)

    def rcopy(src, dst, ss, rs, to):
        return pltpu.make_async_remote_copy(src_ref=src, dst_ref=dst, send_sem=ss, recv_sem=rs,
                                            device_id=dev[to], device_id_type=MESH)

    def al(v, n=128):
        return pl.multiple_of(v, n)

    swaps = {}
    n_sw = [0]

    def swap_start(key, src, dst):
        i = n_sw[0]
        n_sw[0] += 1
        c = rcopy(src, dst, sws_s.at[i], swr_s.at[i], 'c')
        c.start()
        swaps[key] = [c, False]

    def swap_need(key):
        e = swaps[key]
        if not e[1]:
            e[0].wait()
            e[1] = True

    def swap_qkv(l, bs):
        for b in bs:
            for i, w in enumerate((wq, wk, wv)):
                swap_start((l, 'qkv', i, b), w.at[l, pl.ds((1 - core) * HEADS + b * 2, 2)], qkvr.at[l, i, pl.ds(b * 2, 2)])

    def swap_qkv_whole(l):
        for i, w in enumerate((wq, wk, wv)):
            swap_start((l, 'qkv', i), w.at[l, pl.ds((1 - core) * HEADS, HEADS)], qkvr.at[l, i])
            for b in range(N_Q):
                swaps[(l, 'qkv', i, b)] = swaps[(l, 'qkv', i)]

    def swap_gu(l):
        for i, w in enumerate((wg, wu)):
            swap_start((l, 'gu', i), w.at[l, :, pl.ds(al((1 - core) * FHALF), FHALF)], gur.at[l, i])

    steps = []
    for l in range(n_layers):
        for mb in range(2):
            steps += [(l, mb, 'q', b) for b in range(N_Q)]
        for mb in range(2):
            steps += [(l, mb, 'g', b) for b in range(N_G)]

    def w_copies(k):
        l, mb, kind, b = steps[k]
        s = k % 2
        cs = []
        if kind == 'q':
            for i, w in enumerate((wq, wk, wv)):
                for hh in range(2):
                    cols = pl.ds(i * QB + hh * 128, 128)
                    cs.append((w.at[l, core * HEADS + b * 2 + hh], W.at[s, 0, :, cols]))
                    cs.append((qkvr.at[l, i, b * 2 + hh], W.at[s, 1, :, cols]))
        else:
            for i, w in enumerate((wg, wu)):
                cs.append((w.at[l, :, pl.ds(al(core * FHALF + b * GB), GB)], W.at[s, 0, :, pl.ds(i * GB, GB)]))
                cs.append((gur.at[l, i, :, pl.ds(b * GB, GB)], W.at[s, 1, :, pl.ds(i * GB, GB)]))
        return [pltpu.make_async_copy(a, d, w_s.at[s, j]) for j, (a, d) in enumerate(cs)]

    w_live = {}

    def w_start(k):
        if k >= len(steps):
            return
        l, mb, kind, b = steps[k]
        if kind == 'q':
            for i in range(3):
                swap_need((l, 'qkv', i, b))
        else:
            for i in range(2):
                swap_need((l, 'gu', i))
        w_live[k] = w_copies(k)
        for c in w_live[k]:
            c.start()

    x_live = {}

    def issue(k):
        l, mb, kind, b = steps[k]
        s = k % 2
        for c in w_live.pop(k):
            c.wait()
        if k >= 2:
            x_live[k - 2].wait_send()

        def half(j, xs):
            cols = pl.ds(al(j * CB, CB), CB)
            rows = pl.ds(al(xs * ROWS, ROWS), ROWS)
            XP[s, xs, :, cols] = mm(H[mb, rows, :], W[s, 0, :, cols]) + mm(HC[mb, rows, :], W[s, 1, :, cols])
        n = SW // CB
        norm_ready(mb, 1)
        x_live[k] = rcopy(XP.at[s, 1], XR.at[k % 4], xs_s.at[s], xr_s.at[k % 4], 'x')
        if k == 0:
            @pl.loop(0, n)
            def _(j):
                half(j, 1)
            x_live[k].start()
            w_start(1)
            norm_ready(mb, 0)

            @pl.loop(0, n)
            def _(j):
                half(j, 0)
        else:
            norm_ready(mb, 0)

            @pl.loop(0, 2 * n)
            def _(i):
                half(lax.rem(i, n), 1 - lax.div(i, n))

                @pl.when(i == n - 1)
                def _():
                    x_live[k].start()
        w_start(k + 2)

    a_live = {}

    def consume(k):
        l, mb, kind, b = steps[k]
        s, q = k % 2, k % 4
        x_live[k].wait_recv()
        if kind == 'q':

            @pl.loop(0, QB // 128)
            def _(hh):
                def part(i):
                    c = pl.ds(al(i * QB + hh * 128), 128)
                    return XP[s, 0, :, c] + XR[q, :, c]

                def rope(v):
                    return (v * cos_ref[mb] + pltpu.roll(v, 64, 1) * sin_ref[mb]).astype(BF16)
                qh, kh, vh = rope(part(0)), rope(part(1)), part(2).astype(BF16)
                sc = lax.dot_general(qh, kh, (((1,), (1,)), ((), ())), preferred_element_type=F32) * (128 ** -0.5)
                sc = jnp.where(mask_ref[mb] > 0.0, sc, NEG_BIG)
                e = jnp.exp(sc - jnp.max(sc, axis=-1, keepdims=True))
                p = (e / jnp.sum(e, axis=-1, keepdims=True)).astype(BF16)
                ACT[mb, 0, :, pl.ds(al(b * QB + hh * 128), 128)] = mm(p, vh).astype(BF16)
            cols = pl.ds(b * QB, QB)
        else:
            g = XP[s, 0, :, :GB] + XR[q, :, :GB]
            u = XP[s, 0, :, GB:] + XR[q, :, GB:]
            ACT[mb, 0, :, b * GB:(b + 1) * GB] = (jax.nn.silu(g) * u).astype(BF16)
            cols = pl.ds(b * GB, GB)
        c = rcopy(ACT.at[mb, 0, :, cols], ACT.at[mb, 1, :, cols], as_s.at[mb, b], ar_s.at[mb, b], 'x')
        c.start()
        a_live[mb, b] = c

    row_seq = []
    for l in range(n_layers):
        row_seq += [(l, mb, 'o', 0) for mb in range(2)] + [(l, mb, 'd', j) for mb in range(2) for j in range(N_D)]
    row_live = {}

    def row_start(i):
        if i >= len(row_seq):
            return
        l, mb, kind, j = row_seq[i]
        if kind == 'o':
            n, src = HALF, lambda c: wo.at[l, pl.ds(al(c * HALF), HALF), :]
        else:
            n, src = D_CHUNK, lambda c: wd.at[l, pl.ds(al(c * FHALF + j * D_CHUNK), D_CHUNK), :]
        row_live[i] = [pltpu.make_async_copy(src(core), WR.at[0, pl.ds(0, n), :], wr_s.at[0]),
                       pltpu.make_async_copy(src(1 - core), WR.at[1, pl.ds(0, n), :], wr_s.at[1])]
        for c in row_live[i]:
            c.start()

    row_at = [0]

    def row_wait():
        for c in row_live.pop(row_at[0]):
            c.wait()

    def row_done():
        row_at[0] += 1
        row_start(row_at[0])

    def row_mm(mb, xs, a0, n, first):
        @pl.loop(0, FEAT // CB)
        def _(j):
            cols = pl.ds(al(j * CB, CB), CB)
            v = (mm(ACT[mb, xs, :, a0:a0 + n], WR[0, :n, cols])
                 + mm(ACT[mb, 2 + xs, :, a0:a0 + n], WR[1, :n, cols]))
            if first:
                PB[mb, xs, :, cols] = v
            else:
                PB[mb, xs, :, cols] += v

    ac_live = {}

    def act_to_core(mb, xs, j, a0, n):
        cols = pl.ds(a0, n)
        c = rcopy(ACT.at[mb, xs, :, cols], ACT.at[mb, 2 + xs, :, cols], acs_s.at[mb, j, xs], acr_s.at[mb, j, xs], 'c')
        c.start()
        ac_live[mb, j, xs] = c

    y_live = {}

    def y_send(mb, xs, hf):
        cols = pl.ds(hf * (FEAT // 2), FEAT // 2)
        c = rcopy(PB.at[mb, xs, pl.ds(128, 128), cols], YR.at[mb, xs, :, cols], ys_s.at[mb, xs, hf], yr_s.at[mb, xs, hf], 'y')
        c.start()
        y_live[mb, xs, hf] = c

    def r_update(mb, xs, hf):
        y_live[mb, xs, hf].wait()
        rows = slice(xs * 128, xs * 128 + 128)
        cols = slice(hf * (FEAT // 2), (hf + 1) * (FEAT // 2))
        R[mb, rows, cols] = R[mb, rows, cols] + (PB[mb, xs, :128, cols] + YR[mb, xs, :, cols])

    n_live = {}

    def norm_squares(mb):
        acc = None
        for j in range(FEAT // 128):
            v = R[mb, :, j * 128:(j + 1) * 128]
            acc = v * v if acc is None else acc + v * v
        SQ[mb] = jnp.broadcast_to(jnp.sum(acc.T, axis=0, keepdims=True), (8, ROWS))
        c = rcopy(SQ.at[mb], SQC.at[mb], sqcs_s.at[mb], sqcr_s.at[mb], 'c')
        c.start()
        c.wait()
        SQS[mb] = SQ[mb] + SQC[mb]
        c = rcopy(SQS.at[mb], SQX.at[mb], sqxs_s.at[mb], sqxr_s.at[mb], 'x')
        c.start()
        n_live[mb, 'sq'] = c

    def norm_apply(mb, gi):
        n_live[mb, 'sq'].wait()
        g_ref = gm_ref if gi % 2 else ga_ref
        gain = g_ref[gi // 2:gi // 2 + 1, pl.ds(al(t * FEAT), FEAT)].astype(F32)
        for xs in range(2):
            o = 1 - xs
            tot = SQS[mb, 0:1, xs * 128:(xs + 1) * 128] + SQX[mb, 0:1, o * 128:(o + 1) * 128]
            scale = jnp.broadcast_to(lax.rsqrt(tot / EMBED + NORM_EPS), (128, 128)).T[:, 0:1]
            h = R[mb, xs * 128:(xs + 1) * 128, :] * scale * gain
            H[mb, xs * 256:xs * 256 + 128, :] = h.astype(BF16)
        for xs in (1, 0):
            mine, theirs = pl.ds(xs * 256, 128), pl.ds(xs * 256 + 128, 128)
            c = rcopy(H.at[mb, mine, :], H.at[mb, theirs, :], hys_s.at[mb, xs], hyr_s.at[mb, xs], 'y')
            c.start()
            n_live[mb, 'y', xs] = c
        for xs in (1, 0):
            mine = pl.ds(xs * 256, 128)
            c = rcopy(H.at[mb, mine, :], HC.at[mb, mine, :], hcs_s.at[mb, xs], hcr_s.at[mb, xs], 'c')
            c.start()
            n_live[mb, 'c', xs] = c

    def norm_forward(mb, xs):
        if (mb, 'y', xs) in n_live:
            n_live.pop((mb, 'y', xs)).wait()
            theirs = pl.ds(xs * 256 + 128, 128)
            c = rcopy(H.at[mb, theirs, :], HC.at[mb, theirs, :], hcs_s.at[mb, 2 + xs], hcr_s.at[mb, 2 + xs], 'c')
            c.start()
            n_live[mb, 'c', 2 + xs] = c

    def norm_ready(mb, xs):
        norm_forward(mb, xs)
        for i in (xs, 2 + xs):
            if (mb, 'c', i) in n_live:
                n_live.pop((mb, 'c', i)).wait()

    def norm_finish(mb):
        for xs in (1, 0):
            norm_forward(mb, xs)
        for xs in (1, 0):
            norm_ready(mb, xs)

    o_live = []

    def out_send(mb, xs, hf):
        fh = FEAT // 2
        cols = pl.ds(al(t * FEAT + hf * fh), fh)
        for flip in range(2):
            cp = core + flip * (1 - 2 * core)
            src = R.at[mb, pl.ds(al(xs * 128 + cp * 64, 64), 64), pl.ds(hf * fh, fh)]
            to = ('self', 'c', 'x', 'd')[2 * xs + flip]
            i = 2 * xs + flip
            if to == 'self':
                c = pltpu.make_async_copy(src, out_ref.at[mb, :, cols], os_s.at[mb, hf, i])
            else:
                c = rcopy(src, out_ref.at[mb, :, cols], os_s.at[mb, hf, i], or_s.at[mb, hf, i], to)
            c.start()
            o_live.append(c)

    def x_send(mb):
        for i, (k, xs) in enumerate((('x', 1), ('d', 1), ('c', 0), ('self', 0))):
            to_t = {'x': t_x, 'd': t_d, 'c': t_c, 'self': t}[k]
            src = x_ref.at[mb, :, pl.ds(al(to_t * FEAT), FEAT)]
            dst = XB.at[mb, pl.ds(al(xs * 128 + core * 64, 64), 64), :]
            if k == 'self':
                c = pltpu.make_async_copy(src, dst, xbs_s.at[mb, i])
            else:
                c = rcopy(src, dst, xbs_s.at[mb, i], xbr_s.at[mb, i], k)
            c.start()
            n_live[mb, 'xb', i] = c

    def x_take(mb):
        for i in range(4):
            n_live.pop((mb, 'xb', i)).wait()
        R[mb] = XB[mb].astype(F32)

    def seg_send(mb):
        for i, (k, mm_half) in enumerate((('y', 1), ('yc', 1), ('c', 0), ('self', 0))):
            dst = SEG.at[mb, pl.ds(al(mm_half * 128 + core * 64, 64), 64), :]
            if k == 'self':
                c = pltpu.make_async_copy(seg_ref.at[mb], dst, sgs_s.at[mb, i])
            else:
                c = rcopy(seg_ref.at[mb], dst, sgs_s.at[mb, i], sgr_s.at[mb, i], k)
            c.start()
            n_live[mb, 'seg', i] = c

    def tables(mb):
        for i in range(4):
            n_live.pop((mb, 'seg', i)).wait()
        seg = SEG[mb]
        same = None
        for v in ((seg >> 12).astype(F32), (seg & 4095).astype(F32)):
            e = v[:, 0:1] == v.T[0:1, :]
            same = e if same is None else same & e
        r = lax.broadcasted_iota(jnp.int32, (ROWS, ROWS), 0)
        c = lax.broadcasted_iota(jnp.int32, (ROWS, ROWS), 1)

        def place(v):
            return ((v >> 7) ^ m) * 64 + (v & 63)
        same = same & (((r >> 6) & 1) == ((c >> 6) & 1)) & (place(c) <= place(r))
        allowed = jnp.where(same, 1.0, 0.0)
        mask_ref[mb] = allowed
        pos = jnp.sum(allowed, axis=-1, keepdims=True) - 1.0
        lane = lax.broadcasted_iota(jnp.int32, (ROWS, 128), 1).astype(F32)
        pick = jnp.where(lane == pos, 1.0, 0.0)
        for tab, dst in ((ctab_ref, cos_ref), (stab_ref, sin_ref)):
            dst[mb] = jnp.dot(pick, tab[...], preferred_element_type=F32, precision=lax.Precision.HIGHEST)

    todo = {}

    early = {}

    def at(k, f, *args):
        todo.setdefault(k, []).append(functools.partial(f, *args))

    def before(k, f, *args):
        early.setdefault(k, []).append(functools.partial(f, *args))

    def tail_a(l, mb, kind):
        if kind == 'q':
            j, a0, n, first = 0, 0, HALF, True
        else:
            j, a0, n, first = N_D - 1, (N_D - 1) * D_CHUNK, D_CHUNK, False
        act_to_core(mb, 0, j, a0, n)
        row_wait()
        ac_live[mb, j, 0].wait()
        row_mm(mb, 0, a0, n, first)
        y_send(mb, 0, 0)
        if not (l == n_layers - 1 and kind == 'g'):
            y_send(mb, 0, 1)

    def tail_b(l, mb, kind):
        if kind == 'q':
            j, a0, n, first, bs = 0, 0, HALF, True, range(N_Q)
        else:
            j, a0, n, first, bs = N_D - 1, (N_D - 1) * D_CHUNK, D_CHUNK, False, range(N_G - 3, N_G)
        for b in bs:
            a_live[mb, b].wait()
        act_to_core(mb, 1, j, a0, n)
        ac_live[mb, j, 1].wait()
        row_mm(mb, 1, a0, n, first)
        row_done()
        y_send(mb, 1, 0)
        y_send(mb, 1, 1)
        if l == n_layers - 1 and kind == 'g':
            y_send(mb, 0, 1)

    def down_mid(mb, j):
        a0 = j * D_CHUNK
        act_to_core(mb, 0, j, a0, D_CHUNK)
        for b in range(3 * j, 3 * j + 3):
            a_live[mb, b].wait()
        act_to_core(mb, 1, j, a0, D_CHUNK)
        row_wait()
        for xs in range(2):
            ac_live[mb, j, xs].wait()

        @pl.loop(0, 2)
        def _(xs):
            row_mm(mb, xs, a0, D_CHUNK, j == 0)
        row_done()

    def update_and_squares(mb):
        for xs in range(2):
            for hf in range(2):
                r_update(mb, xs, hf)
        norm_squares(mb)

    pieces = ((1, 0), (1, 1), (0, 0), (0, 1))

    def finish(mb):
        for xs, hf in pieces:
            r_update(mb, xs, hf)

    def send_finished(mb):
        for xs, hf in pieces:
            out_send(mb, xs, hf)

    def finish_out(mb):
        for xs, hf in pieces:
            r_update(mb, xs, hf)
            out_send(mb, xs, hf)

    def first_squares(mb):
        x_take(mb)
        norm_squares(mb)

    n_steps = len(steps)
    at(n_steps, send_finished, 0)
    for k, (l, mb, kind, b) in enumerate(steps):
        last = b == (N_Q if kind == 'q' else N_G) - 1
        if kind == 'g' and b % 3 == 2 and not last:
            before(k + 3, down_mid, mb, b // 3)
        if last:
            before(k + 2, tail_a, l, mb, kind)
            before(k + 3, tail_b, l, mb, kind)
            if kind == 'g' and l == n_layers - 1:
                at(k + 3, finish if mb == 0 else finish_out, mb)
            else:
                at(k + 3, update_and_squares, mb)
                at(k + 4, norm_apply, mb, 2 * l + 1 if kind == 'q' else 2 * l + 2)
                at(k + 5, norm_finish, mb)
    at(0, tables, 0)
    at(1, first_squares, 1)
    at(4, tables, 1)
    at(2, norm_apply, 1, 0)
    at(3, norm_finish, 1)
    at(3, swap_gu, 0)
    if n_layers > 1:
        at(2 * N_Q + 7, swap_qkv_whole, 1)
        at(2 * N_Q + 12, swap_gu, 1)

    x_send(0)
    for mb in range(2):
        seg_send(mb)
    swap_qkv(0, (0,))
    row_start(0)
    first_squares(0)
    x_send(1)
    w_start(0)
    norm_apply(0, 0)
    swap_qkv(0, range(1, N_Q))
    for k in range(n_steps + 4):
        if k < n_steps:
            issue(k)
        for f in early.pop(k, []):
            f()
        if 1 <= k <= n_steps:
            consume(k - 1)
        for f in todo.pop(k, []):
            f()
    assert not todo and not early
    for k in (n_steps - 2, n_steps - 1):
        x_live[k].wait_send()
    for c in o_live:
        c.wait()


def solution(mesh):
    act_spec = P(None, ('rep', 'tok', 'mp'), None)
    seg_spec = P(None, ('rep', 'tok', 'mp'))
    gain_spec = P(None, None)
    head_in = P(None, 'tok', 'mp', None)
    head_out = P(None, 'mp', None, 'tok')
    ffn_in = P(None, 'tok', 'mp')
    ffn_out = P(None, 'mp', 'tok')

    def device_fn(x_in, seg_ids, g_attn, w_q, w_k, w_v, w_o, g_mlp, w_gate, w_up, w_down):
        n_layers = w_q.shape[0]
        micro_n, loc_len, embed = x_in.shape
        feat, heads, head_dim = w_q.shape[1:]
        seg_b = jnp.broadcast_to(seg_ids[:, :, None], (micro_n, loc_len, 128))
        cos_rows, sin_rows = rope_rows(2 * loc_len, head_dim)
        by_head = [w.transpose(0, 2, 1, 3) for w in (w_q, w_k, w_v)]
        flat_o = w_o.reshape(n_layers, heads * head_dim, feat)

        vm = pl.BlockSpec(memory_space=pltpu.VMEM)
        hb = pl.BlockSpec(memory_space=pltpu.HBM)
        dma = pltpu.SemaphoreType.DMA
        out = pl.pallas_call(
            functools.partial(body, n_layers),
            out_shape=(jax.ShapeDtypeStruct((micro_n, loc_len, embed), F32),
                       jax.ShapeDtypeStruct((n_layers, 3, HEADS, FEAT, 128), BF16),
                       jax.ShapeDtypeStruct((n_layers, 2, FEAT, FHALF), BF16)),
            in_specs=[hb] * 2 + [vm] * 4 + [hb] * 7,
            out_specs=(hb, hb, hb),
            scratch_shapes=[
                pltpu.VMEM((2, ROWS, 128), jnp.int32),
                pltpu.VMEM((2, ROWS, 128), F32),
                pltpu.VMEM((2, ROWS, 128), F32),
                pltpu.VMEM((2, ROWS, ROWS), F32),
                pltpu.VMEM((2, 256, FEAT), BF16),
                pltpu.VMEM((2, 256, FEAT), F32),
                pltpu.VMEM((2, 512, FEAT), BF16),
                pltpu.VMEM((2, 512, FEAT), BF16),
                pltpu.VMEM((2, 2, ROWS, SW), F32),
                pltpu.VMEM((4, ROWS, SW), F32),
                pltpu.VMEM((2, 2, FEAT, SW), BF16),
                pltpu.VMEM((2, HALF, FEAT), BF16),
                pltpu.VMEM((2, 4, ROWS, FHALF), BF16),
                pltpu.VMEM((2, 2, ROWS, FEAT), F32),
                pltpu.VMEM((2, 2, 128, FEAT), F32),
                pltpu.VMEM((2, 8, ROWS), F32),
                pltpu.VMEM((2, 8, ROWS), F32),
                pltpu.VMEM((2, 8, ROWS), F32),
                pltpu.VMEM((2, 8, ROWS), F32),
                dma((2,)), dma((4,)),
                dma((2, N_G)), dma((2, N_G)),
                dma((2, N_D, 2)), dma((2, N_D, 2)),
                dma((2, 2, 2)), dma((2, 2, 2)),
                dma((2, 2)), dma((2, 2)),
                dma((2, 4)), dma((2, 4)),
                dma((2,)), dma((2,)), dma((2,)), dma((2,)),
                dma((22,)), dma((22,)),
                dma((2, 2, 4)), dma((2, 2, 4)),
                dma((2, 4)), dma((2, 4)),
                dma((2, 4)), dma((2, 4)),
                dma((2, 12)), dma((2,)),
            ],
            compiler_params=pltpu.CompilerParams(collective_id=0, has_side_effects=True, vmem_limit_bytes=67043328),
        )(x_in, seg_b, cos_rows, sin_rows, g_attn, g_mlp, *by_head, flat_o, w_gate, w_up, w_down)
        return out[0]

    return jax.shard_map(
        device_fn,
        mesh=mesh,
        in_specs=(act_spec, seg_spec, gain_spec, head_in, head_in, head_in, head_out, gain_spec, ffn_in, ffn_in, ffn_out),
        out_specs=act_spec,
        check_vma=False,
    )
```
